256 devices in a mesh: dp: 16 (over y_hi, x, core), mp: 16 (over z, y_lo).
Axes of the slice: x: 4, y: 4 (y_hi: 2, y_lo: 2; y = y_hi * 2 + y_lo), z: 8, core: 2. Of those that a mesh axis runs over, the one named last changes fastest.
Arguments:
- tokens: bfloat16 [8192, 8192], P(('dp', 'mp')), parts along dimension 0, may hold values from -6 to 6
- norm_gain: float32 [8192], replicated, may hold values from 0.5 to 1.5
- qkv_weight: bfloat16 [8192, 10240], P(None, 'mp'), may hold values from -0.0625 to 0.0625
- qkv_bias: float32 [10240], P('mp'), may hold values from -3 to 3
- qkv_grad: bfloat16 [8192, 10240], P('dp', 'mp'), parts along dimension 0, may hold values from -6 to 6
Outputs:
- qkv: bfloat16 [8192, 10240], P('dp', 'mp'), parts along dimension 0
- tokens_grad: float32 [8192, 8192], P(('dp', 'mp')), parts along dimension 0
- gain_grad: float32 [131072], P('dp'), parts along dimension 0
- bias_grad: float32 [163840], P(('dp', 'mp')), parts along dimension 0
The draws below stay inside these ranges and needn't reach their ends.
There are 16 independent parts, one for each index of `dp`. The reference program is written for one: setup_inputs(seed, part) draws one part's arguments, and reference() takes and returns one part's arrays. A program takes and returns all parts, laid end to end along the dimension named above; an argument that names none is the same for every part. Nothing has to cross between parts.
All inputs are finite; a program needn't handle non-finite values.
Results may differ from the reference program's by a relative error of at most 0.0046.
Values may be sent and summed in bfloat16 or wider, within the bound.
No kernel may reach another device: no remote copies, remote signals or barrier semaphores. Data moves between devices by JAX's collectives and lax.ppermute only.
A program may use at most 128 MiB of HBM per device.

```python
import jax
import jax.numpy as jnp
from jax import lax

D = 8192
HEAD_DIM = 128
GROUP = 10
COLS = 10240
STRIDE = 2048
TOK_DEV = 32
TOKENS = 512


def strengthened(values, own_key, source, target, shards_of, factor):
    def block_of(axis_at):
        return (jnp.arange(values.shape[axis_at]) // (values.shape[axis_at] // shards_of)).reshape((-1,) + (1,) * (values.ndim - 1 - axis_at))

    first = jax.random.permutation(own_key, shards_of)[block_of(target)]
    far = (block_of(target) + shards_of // 2) % shards_of
    return jnp.where((block_of(source) == first) | (block_of(source) == far), factor * values, values)


def shard_levels(stream_key, shape, cuts, smallest, top_value):
    def one(axis_at, blocks):
        heights = jax.random.uniform(jax.random.fold_in(jax.random.fold_in(stream_key, 6), axis_at), (blocks,), jnp.float32, smallest / len(cuts), top_value / len(cuts))
        return jnp.repeat(jnp.exp(heights), shape[axis_at] // blocks).reshape((-1,) + (1,) * (len(shape) - axis_at - 1))

    factor_of = one(*cuts[0])
    for cut in cuts[1:]:
        factor_of = factor_of * one(*cut)
    return factor_of


def gaussian(own_key, dims, deviation, bound, shards=(), kind=jnp.bfloat16):
    array = deviation * jax.random.normal(own_key, dims, jnp.float32)
    if shards:
        array = array * shard_levels(own_key, dims, shards, -0.22, 0.18)
    return jnp.clip(array, -bound, bound).astype(kind)


def gaussian_with(stream_key, extent, deviation, limit, cuts, heavy, kind=jnp.bfloat16):
    array = deviation * jax.random.normal(stream_key, extent, jnp.float32)
    if cuts:
        array = array * shard_levels(stream_key, extent, cuts, -0.22, 0.18)
    return jnp.clip(strengthened(array, jax.random.fold_in(stream_key, 3), *heavy), -limit, limit).astype(kind)


def setup_inputs(seed: int = 0, part: int = 0) -> dict:
    key_list = jax.random.split(jax.random.key(seed), 6)
    part_keys = jax.random.split(jax.random.fold_in(key_list[5], part), 6)
    return {
        "tokens": gaussian(part_keys[0], (TOKENS, D), 1.0, 6.0, ((0, 16),)),
        "norm_gain": jnp.clip(1.0 + 0.1 * jax.random.normal(key_list[1], (D,), jnp.float32), 0.5, 1.5),
        "qkv_weight": gaussian(key_list[2], (D, COLS), D ** -0.5, 0.0625, ((1, 16),)),
        "qkv_bias": gaussian(key_list[3], (COLS,), 0.5, 3.0, ((0, 16),), jnp.float32),
        "qkv_grad": gaussian_with(part_keys[4], (TOKENS, COLS), 1.0, 6.0, ((1, 16),), (1, 0, 16, 2.0)),
    }


def rotate_heads(joined, first_col, position, sign):
    rows, cols = joined.shape
    heads = cols // HEAD_DIM
    half = HEAD_DIM // 2
    parts = joined.reshape(rows, heads, 2, half)
    inverse = jnp.exp(-jnp.log(jnp.float32(1000000.0)) * (2.0 * jnp.arange(half).astype(jnp.float32) / HEAD_DIM))
    angle = position.astype(jnp.float32)[:, None] * inverse[None, :]
    cosine = jnp.cos(angle)[:, None, :]
    sine = sign * jnp.sin(angle)[:, None, :]
    first = parts[:, :, 0, :]
    second = parts[:, :, 1, :]
    turned = jnp.stack([first * cosine - second * sine, second * cosine + first * sine], axis=2)
    head_index = first_col // HEAD_DIM + jnp.arange(heads)
    rotated = head_index % GROUP != GROUP - 1
    result = jnp.where(rotated[None, :, None, None], turned, parts)
    return result.reshape(rows, cols)

def reference(tokens, norm_gain, qkv_weight, qkv_bias, qkv_grad):
    row_index = jnp.arange(TOKENS).astype(jnp.int32)
    position = row_index // TOK_DEV * STRIDE + row_index % TOK_DEV
    values = tokens.astype(jnp.float32)
    scale = lax.rsqrt(lax.optimization_barrier(jnp.mean(values * values, axis=1, keepdims=True)) + 1e-06)
    normed = (values * scale * norm_gain[None, :]).astype(jnp.bfloat16)
    joined = jnp.dot(normed, qkv_weight, preferred_element_type=jnp.float32) + qkv_bias[None, :]
    qkv = rotate_heads(joined, 0, position, 1.0).astype(jnp.bfloat16)
    joined_grad = rotate_heads(qkv_grad.astype(jnp.float32), 0, position, -1.0)
    bias_grad = lax.optimization_barrier(jnp.sum(joined_grad, axis=0))
    joined_low = joined_grad.astype(jnp.bfloat16)
    normed_grad = lax.dot_general(joined_low, qkv_weight, (((1,), (1,)), ((), ())), preferred_element_type=jnp.float32)
    gain_grad = lax.optimization_barrier(jnp.sum(normed_grad * values * scale, axis=0))
    inner = lax.optimization_barrier(jnp.mean(norm_gain[None, :] * normed_grad * values, axis=1, keepdims=True))
    tokens_grad = scale * norm_gain[None, :] * normed_grad - values * scale * scale * scale * inner
    return (qkv, tokens_grad, gain_grad, bias_grad)
```

```python
import functools

import jax
import jax.numpy as jnp
from jax import lax
from jax.experimental import pallas as pl
from jax.experimental.pallas import tpu as pltpu
from jax.sharding import Mesh
from jax.sharding import PartitionSpec as P

HEAD_DIM = 128
SEQ_LEN = 32768
GROUP = 10
TOK_DEV = 32
PAIR = 2 * TOK_DEV
RING = 8
MP = ("mp_0", "mp_1")
DP_MP = ("dp", "mp_0", "mp_1")
UP = [(i, (i + 1) % RING) for i in range(RING)]
DOWN = [(i, (i - 1) % RING) for i in range(RING)]
SWAP = [(0, 1), (1, 0)]
KBLK = 1024
HALVES = 2
CBLK = 512
NBLK = 256
UP_FAR = 2048
CUT = 5120


def up(value):
    return lax.ppermute(value, "mp_0", UP)


def down(value):
    return lax.ppermute(value, "mp_0", DOWN)


def swap(value):
    return lax.ppermute(value, "mp_1", SWAP)


def tables(rows, stride):
    half = HEAD_DIM // 2
    row_index = jnp.arange(rows)
    place = row_index // TOK_DEV * stride + row_index % TOK_DEV
    inverse = jnp.exp(
        -jnp.log(jnp.float32(1000000.0)) * (2.0 * jnp.arange(half).astype(jnp.float32) / HEAD_DIM)
    )
    angle = place.astype(jnp.float32)[:, None] * inverse[None, :]
    cosine, sine = jnp.cos(angle), jnp.sin(angle)
    return (
        jnp.concatenate([cosine, cosine], axis=1),
        jnp.concatenate([-sine, sine], axis=1),
    )


def turn(value, cosine, sine, straight):
    cosine = jnp.where(straight, 1.0, cosine)
    sine = jnp.where(straight, 0.0, sine)
    return value * cosine + pltpu.roll(value, HEAD_DIM // 2, 1) * sine


def params(mib):
    return pltpu.CompilerParams(vmem_limit_bytes=mib << 20)


def in_vmem(value):
    return pltpu.with_memory_space_constraint(value, pltpu.VMEM)


VMEM_SPEC = pl.BlockSpec(memory_space=pltpu.VMEM)
SMEM_SPEC = pl.BlockSpec(memory_space=pltpu.SMEM)
ANY_SPEC = pl.BlockSpec(memory_space=pl.ANY)


def over_weight(weight_ref, first, count, body):
    def step(at, carry):
        body(at, weight_ref[pl.ds(pl.multiple_of((first + at) * KBLK, KBLK), KBLK), :])
        return carry

    lax.fori_loop(0, count, step, 0)


def over_copied(weight_ref, buffer_ref, sem, count, body):
    def copy(at):
        rows = pl.ds(pl.multiple_of(at * KBLK, KBLK), KBLK)
        return pltpu.make_async_copy(weight_ref.at[rows, :], buffer_ref.at[at % 2], sem.at[at % 2])

    copy(0).start()

    def step(at, carry):
        @pl.when(at + 1 < count)
        def _():
            copy(at + 1).start()

        copy(at).wait()
        body(at, buffer_ref[at % 2])
        return carry

    lax.fori_loop(0, count, step, 0)


def product(over, low_ref, out_ref):
    def body(at, block):
        lanes = pl.ds(pl.multiple_of(at * KBLK, KBLK), KBLK)
        out_ref[:, lanes] = lax.dot_general(
            low_ref[...], block, (((1,), (1,)), ((), ())), preferred_element_type=jnp.float32
        )

    over(out_ref.shape[1] // KBLK, body)


def rotate_kernel(spots, grad_ref, cos_ref, sin_ref, weight_ref, out_ref, low_ref, bias_ref, *scratch):
    for head in range(grad_ref.shape[1] // HEAD_DIM):
        lanes = pl.ds(head * HEAD_DIM, HEAD_DIM)
        value = grad_ref[:, lanes].astype(jnp.float32)
        turned = turn(value, cos_ref[...], -sin_ref[...], spots[2 + head] == 1)
        bias_ref[:, lanes] = jnp.sum(turned, axis=0, keepdims=True)
        low_ref[:, lanes] = turned.astype(jnp.bfloat16)
    product(functools.partial(over_copied, weight_ref, *scratch), low_ref, out_ref)


def back_first(spots, grad, cosine, sine, weight):
    rows, cols = grad.shape
    return pl.pallas_call(
        rotate_kernel,
        in_specs=[SMEM_SPEC] + [VMEM_SPEC] * 3 + [ANY_SPEC],
        out_specs=[VMEM_SPEC] * 3,
        out_shape=[
            pltpu.VMEM((rows, weight.shape[0] // HALVES), jnp.float32),
            pltpu.VMEM((rows, cols), jnp.bfloat16),
            jax.ShapeDtypeStruct((1, cols), jnp.float32),
        ],
        scratch_shapes=[pltpu.VMEM((2, KBLK, cols), jnp.bfloat16), pltpu.SemaphoreType.DMA((2,))],
        compiler_params=params(6),
        name="back_first",
    )(spots, grad, cosine, sine, pltpu.with_memory_space_constraint(weight, pltpu.HBM))


def second_kernel(low_ref, weight_ref, out_ref):
    product(functools.partial(over_weight, weight_ref, out_ref.shape[1] // KBLK), low_ref, out_ref)


def back_second(low, weight):
    rows, _ = low.shape
    return pl.pallas_call(
        second_kernel,
        in_specs=[VMEM_SPEC] * 2,
        out_specs=VMEM_SPEC,
        out_shape=pltpu.VMEM((rows, weight.shape[0] // HALVES), jnp.float32),
        compiler_params=params(4),
        name="back_second",
    )(low, in_vmem(weight))


def over_columns(start, stop, body, block=CBLK):
    def step(at, carry):
        body(pl.multiple_of(start + at * block, block))
        return carry

    lax.fori_loop(0, (stop - start) // block, step, 0)


def away(spots, offset):
    return lax.rem(spots[0] + (offset + RING), RING)


def add_kernel(jobs, spots, first_ref, second_ref, *refs):
    half = first_ref.shape[1]
    arrived, outs = refs[: -len(jobs)], refs[-len(jobs) :]
    for (offset, (start, stop), taken), out_ref in zip(jobs, outs):
        rows = pl.ds(pl.multiple_of(away(spots, offset) * PAIR, PAIR), PAIR)
        spans = [span for _, span in taken]
        edges = {start, stop} | {e for span in ((half, half), *spans) for e in span if start < e < stop}
        edges = sorted(edges)
        for low, high in zip(edges[:-1], edges[1:]):
            source, base = (first_ref, 0) if low < half else (second_ref, half)
            adds = [(arrived[at], span[0]) for at, span in taken if span[0] <= low < span[1]]

            def body(at):
                total = source[rows, pl.ds(at - base, CBLK)]
                for ref, begin in adds:
                    total = total + ref[:, pl.ds(at - begin, CBLK)].astype(jnp.float32)
                out_ref[:, pl.ds(at - start, CBLK)] = total.astype(jnp.bfloat16)

            over_columns(low, high, body)


def added(spots, partials, jobs, arrived):
    return pl.pallas_call(
        functools.partial(add_kernel, jobs),
        in_specs=[SMEM_SPEC] + [VMEM_SPEC] * (2 + len(arrived)),
        out_specs=[VMEM_SPEC] * len(jobs),
        out_shape=[pltpu.VMEM((PAIR, stop - start), jnp.bfloat16) for _, (start, stop), _ in jobs],
        compiler_params=params(2),
        name="add",
    )(spots, *partials, *[in_vmem(value) for value in arrived])


def join_kernel(bounds, spots, first_ref, second_ref, rising_ref, falling_ref, mine_ref, other_ref):
    first, stop = bounds
    half = first_ref.shape[1]
    for at, out_ref in ((spots[1], mine_ref), (1 - spots[1], other_ref)):
        local = pl.ds(pl.multiple_of(at * TOK_DEV, TOK_DEV), TOK_DEV)
        whole = pl.ds(pl.multiple_of(spots[0] * PAIR + at * TOK_DEV, TOK_DEV), TOK_DEV)
        for source, low, high in ((first_ref, 0, half), (second_ref, half, 2 * half)):

            def body(start):
                lanes = pl.ds(start - first, CBLK)
                total = source[whole, pl.ds(start - low, CBLK)] + rising_ref[local, lanes].astype(jnp.float32)
                total = total + falling_ref[local, lanes].astype(jnp.float32)
                out_ref[:, lanes] = total.astype(out_ref.dtype)

            if max(first, low) < min(stop, high):
                over_columns(max(first, low), min(stop, high), body)


def joined(spots, partials, bounds, rising, falling):
    span = bounds[1] - bounds[0]
    return pl.pallas_call(
        functools.partial(join_kernel, bounds),
        in_specs=[SMEM_SPEC] + [VMEM_SPEC] * 4,
        out_specs=[VMEM_SPEC] * 2,
        out_shape=[
            pltpu.VMEM((TOK_DEV, span), jnp.float32),
            pltpu.VMEM((TOK_DEV, span), jnp.bfloat16),
        ],
        compiler_params=params(2),
        name="join",
    )(spots, *partials, in_vmem(rising), in_vmem(falling))


def sum_kernel(left_ref, right_ref, out_ref):
    out_ref[...] = left_ref[...] + right_ref[...]


def summed(left, right):
    return pl.pallas_call(
        sum_kernel,
        in_specs=[VMEM_SPEC] * 2,
        out_specs=VMEM_SPEC,
        out_shape=jax.ShapeDtypeStruct(left.shape, left.dtype),
        compiler_params=params(2),
        name="sum",
    )(left, right)


def finish_kernel(x_ref, gain_ref, mine0, other0, mine1, other1, out_ref):
    width = x_ref.shape[1]
    first = mine0.shape[1]
    squares = jnp.zeros((TOK_DEV, HEAD_DIM), jnp.float32)
    products = jnp.zeros((TOK_DEV, HEAD_DIM), jnp.float32)

    def at(start):
        mine, other, base = (mine0, other0, 0) if start < first else (mine1, other1, first)
        local = pl.ds(start - base, HEAD_DIM)
        grad = mine[:, local] + other[:, local].astype(jnp.float32)
        lanes = pl.ds(start, HEAD_DIM)
        return x_ref[:, lanes].astype(jnp.float32), gain_ref[:, lanes] * grad, lanes

    for start in range(0, width, HEAD_DIM):
        value, grad, _ = at(start)
        squares = squares + value * value
        products = products + grad * value
    scale = lax.rsqrt(jnp.sum(squares, axis=1, keepdims=True) / width + 1e-06)
    inner = scale * scale * scale * (jnp.sum(products, axis=1, keepdims=True) / width)
    for start in range(0, width, HEAD_DIM):
        value, grad, lanes = at(start)
        out_ref[:, lanes] = scale * grad - value * inner


def finished(tokens, gain, parts):
    return pl.pallas_call(
        finish_kernel,
        out_shape=jax.ShapeDtypeStruct(tokens.shape, jnp.float32),
        compiler_params=params(8),
        name="finish",
    )(tokens, gain, *parts)


def token_rows(spots, shift, swapped):
    side = 1 - spots[1] if swapped else spots[1]
    block = away(spots, shift) * (PAIR // TOK_DEV) + side
    return pl.ds(pl.multiple_of(block * TOK_DEV, TOK_DEV), TOK_DEV)


def norm_kernel(marks, spots, *refs):
    count = len(marks)
    xs, refs = refs[:count], refs[count:]
    first_ref, second_ref, gain_ref, refs = *refs[:3], refs[3:]
    normed_ref, total_ref = refs[-2:]
    width = gain_ref.shape[1]
    half = first_ref.shape[1]
    scales = []
    for j in range(count):

        def squares(at, total):
            for lane in range(0, CBLK, HEAD_DIM):
                lanes = pl.ds(pl.multiple_of(at * CBLK + lane, HEAD_DIM), HEAD_DIM)
                value = xs[j][:, lanes].astype(jnp.float32)
                total = total + value * value
            return total

        total = lax.fori_loop(0, width // CBLK, squares, jnp.zeros((TOK_DEV, HEAD_DIM), jnp.float32))
        scales.append(lax.rsqrt(jnp.sum(total, axis=1, keepdims=True) / width + 1e-06))

    for source, start in ((first_ref, 0), (second_ref, half)):

        def body(at):
            lanes = pl.ds(at, NBLK)
            gain = gain_ref[:, lanes]
            products = jnp.zeros((TOK_DEV, NBLK), jnp.float32)
            for j, mark in enumerate(marks):
                value = xs[j][:, lanes].astype(jnp.float32) * scales[j]
                products = products + source[token_rows(spots, *mark), pl.ds(at - start, NBLK)] * value
                normed_ref[j * TOK_DEV : (j + 1) * TOK_DEV, lanes] = (value * gain).astype(jnp.bfloat16)
            total = jnp.sum(products, axis=0, keepdims=True)
            if len(refs) > 2:
                total = total + refs[0][:, lanes]
            total_ref[:, lanes] = total

        over_columns(start, start + half, body, NBLK)


def normalized(marks, spots, pieces, partials, gain, carried):
    count = len(pieces)
    width = gain.shape[1]
    return pl.pallas_call(
        functools.partial(norm_kernel, marks),
        in_specs=[SMEM_SPEC] + [VMEM_SPEC] * (count + 3 + len(carried)),
        out_specs=[VMEM_SPEC] * 2,
        out_shape=[
            pltpu.VMEM((count * TOK_DEV, width), jnp.bfloat16),
            pltpu.VMEM((1, width), jnp.float32),
        ],
        compiler_params=params(2),
        name="norm",
    )(spots, *[in_vmem(piece) for piece in pieces], *partials, gain, *carried)


def project_kernel(marks, spots, *refs):
    groups = len(marks)
    normed, refs = refs[:groups], refs[groups:]
    weight_ref, bias_ref, cos_ref, sin_ref = refs[:4]
    out_ref, acc_ref, stage_ref, out_sem = refs[-4:]
    acc_ref[...] = jnp.zeros_like(acc_ref)

    def body(at, block):
        lanes = pl.ds(pl.multiple_of(at * KBLK, KBLK), KBLK)
        values = [ref[:, lanes] for ref in normed]
        value = values[0] if groups == 1 else jnp.concatenate(values, axis=0)
        acc_ref[...] += jnp.dot(value, block, preferred_element_type=jnp.float32)

    over_weight(weight_ref, 0, weight_ref.shape[0] // KBLK, body)
    copies = []
    for j, mark in enumerate(mark for group in marks for mark in group):
        rows = pl.ds(j * TOK_DEV, TOK_DEV)
        whole = token_rows(spots, *mark)
        for head in range(stage_ref.shape[1] // HEAD_DIM):
            lanes = pl.ds(head * HEAD_DIM, HEAD_DIM)
            value = acc_ref[rows, lanes] + bias_ref[:, lanes]
            stage_ref[rows, lanes] = turn(
                value, cos_ref[whole, :], sin_ref[whole, :], spots[2 + head] == 1
            ).astype(jnp.bfloat16)
        copy = pltpu.make_async_copy(stage_ref.at[rows, :], out_ref.at[whole, :], out_sem.at[j])
        copy.start()
        copies.append(copy)
    for copy in copies:
        copy.wait()


def project(marks, spots, normed, weight, bias, cosine, sine, carried):
    rows, cols = sum(part.shape[0] for part in normed), weight.shape[1]
    in_specs = [SMEM_SPEC] + [VMEM_SPEC] * (len(normed) + 4)
    return pl.pallas_call(
        functools.partial(project_kernel, marks),
        in_specs=in_specs + [ANY_SPEC] * len(carried),
        out_specs=ANY_SPEC,
        out_shape=pltpu.HBM((cosine.shape[0], cols), jnp.bfloat16),
        scratch_shapes=[
            pltpu.VMEM((rows, cols), jnp.float32),
            pltpu.VMEM((rows, cols), jnp.bfloat16),
            pltpu.SemaphoreType.DMA((rows // TOK_DEV,)),
        ],
        input_output_aliases={len(in_specs): 0} if carried else {},
        compiler_params=params(4),
        name="project",
    )(spots, *normed, in_vmem(weight), bias, cosine, sine, *carried)


def work(tokens, norm_gain, qkv_weight, qkv_bias, qkv_grad):
    width, cols = qkv_weight.shape
    rows = qkv_grad.shape[0]
    heads = cols // HEAD_DIM
    ring = lax.axis_index("mp_0")
    side = lax.axis_index("mp_1")
    first_head = lax.axis_index(MP) * heads
    straight = ((first_head + jnp.arange(heads)) % GROUP == GROUP - 1).astype(jnp.int32)
    spots = jnp.concatenate([jnp.stack([ring, side]).astype(jnp.int32), straight])
    cosine, sine = tables(rows, SEQ_LEN // lax.axis_size(MP))
    spots, cosine, sine, gain_row, bias_row, qkv_grad = lax.optimization_barrier(
        (spots, cosine, sine, norm_gain[None, :], qkv_bias[None, :], qkv_grad)
    )
    cosine, sine, gain_row, bias_row = map(in_vmem, (cosine, sine, gain_row, bias_row))

    ups, downs = [tokens], [tokens]
    for _ in range(1, RING // 2 + 1):
        ups.append(up(ups[-1]))
    for _ in range(1, RING // 2):
        downs.append(down(downs[-1]))
    near = {"0": (0, tokens, swap(tokens))}
    for step in range(1, RING // 2 + 1):
        near[f"{step}u"] = (-step, ups[step], swap(ups[step]))
        if step < RING // 2:
            near[f"{step}d"] = (step, downs[step], swap(downs[step]))

    first, low, bias_grad = back_first(spots, qkv_grad, cosine, sine, qkv_weight)
    partials = (in_vmem(first), in_vmem(back_second(low, qkv_weight)))

    half = width // HALVES
    cut_a, cut_b, rest = (0, CUT), (CUT, width), (half, width)
    far_u, far_d = (0, UP_FAR), (UP_FAR, half)
    early = partials[:1] * 2

    def taken(at, span):
        return ((at, span),)

    rising, falling = added(spots, early, ((4, far_u, ()), (-4, far_d, ())), ())
    up4, down4a = up(rising), down(falling)
    (falling,) = added(spots, partials, ((-4, rest, ()),), ())
    down4b = down(falling)
    (rising,) = added(spots, partials, ((3, cut_a, taken(0, far_u)),), (up4,))
    up3a = up(rising)
    rising, falling = added(
        spots, partials, ((3, cut_b, ()), (-3, cut_a, taken(0, far_d) + taken(1, rest))), (down4a, down4b)
    )
    up3b, down3a = up(rising), down(falling)
    (falling,) = added(spots, partials, ((-3, cut_b, taken(0, rest)),), (down4b,))
    down3b = down(falling)
    rising, falling, later = added(
        spots,
        partials,
        ((2, cut_a, taken(0, cut_a)), (-2, cut_a, taken(1, cut_a)), (2, cut_b, taken(2, cut_b))),
        (up3a, down3a, up3b),
    )
    up2a, down2a, up2b = up(rising), down(falling), up(later)
    (falling,) = added(spots, partials, ((-2, cut_b, taken(0, cut_b)),), (down3b,))
    down2b = down(falling)
    parts = []
    for span, rising, falling in ((cut_a, up2a, down2a), (cut_b, up2b, down2b)):
        rising, falling = added(
            spots, partials, ((1, span, taken(0, span)), (-1, span, taken(1, span))), (rising, falling)
        )
        rising, falling = up(rising), down(falling)
        mine, other = joined(spots, partials, span, rising, falling)
        parts += [mine, swap(other)]

    sums, batches = (), []
    for names in (("0", "1u"), ("1d", "2u"), ("2d", "3u"), ("3d", "4u")):
        group = [near[name] for name in names]
        pieces = [piece for _, piece, _ in group] + [piece for _, _, piece in group]
        marks = tuple((shift, swapped) for swapped in (False, True) for shift, _, _ in group)
        normed, total = normalized(marks, spots, pieces, partials, gain_row, sums)
        sums = (total,)
        batches.append((marks, normed))
    out = ()
    for batch in (batches[:1], batches[1:2], batches[2:]):
        marks, normed = zip(*batch)
        out = (
            project(marks, spots, normed, qkv_weight, bias_row, cosine, sine, out),
        )

    total = summed(total, swap(total))
    for reach in (4, 1, 2):
        pairs = [(i, i ^ reach) for i in range(RING)]
        total = summed(total, lax.ppermute(total, "mp_0", pairs))

    bias_grad, parts[2] = lax.optimization_barrier((bias_grad, parts[2]))
    tokens_grad = finished(tokens, gain_row, parts)
    return (out[0], tokens_grad, total[0], bias_grad[0])


def solution(mesh):
    split = Mesh(mesh.devices.reshape(mesh.shape["dp"], 8, 2), ("dp", "mp_0", "mp_1"))
    placed = (P(DP_MP, None), P(), P(None, MP), P(MP), P("dp", MP))
    return jax.shard_map(
        work,
        mesh=split,
        in_specs=placed,
        out_specs=(P("dp", MP), P(DP_MP, None), P("dp"), P(DP_MP)),
        check_vma=False,
    )
```

```python
import functools

import jax
import jax.numpy as jnp
from jax import lax
from jax.experimental import pallas as pl
from jax.experimental.pallas import tpu as pltpu
from jax.sharding import Mesh
from jax.sharding import PartitionSpec as P

HEAD_DIM = 128
SEQ_LEN = 32768
GROUP = 10
TOK_DEV = 32
PAIR = 2 * TOK_DEV
RING = 8
MP = ("mp_0", "mp_1")
DP_MP = ("dp", "mp_0", "mp_1")
UP = [(i, (i + 1) % RING) for i in range(RING)]
DOWN = [(i, (i - 1) % RING) for i in range(RING)]
SWAP = [(0, 1), (1, 0)]
KBLK = 1024
HALVES = 2
CBLK = 512
NBLK = 256
UP_FAR = 2304
CUT = 5632


def up(value):
    return lax.ppermute(value, "mp_0", UP)


def down(value):
    return lax.ppermute(value, "mp_0", DOWN)


def swap(value):
    return lax.ppermute(value, "mp_1", SWAP)


def tables(rows, stride):
    half = HEAD_DIM // 2
    row_index = jnp.arange(rows)
    place = row_index // TOK_DEV * stride + row_index % TOK_DEV
    inverse = jnp.exp(
        -jnp.log(jnp.float32(1000000.0)) * (2.0 * jnp.arange(half).astype(jnp.float32) / HEAD_DIM)
    )
    angle = place.astype(jnp.float32)[:, None] * inverse[None, :]
    cosine, sine = jnp.cos(angle), jnp.sin(angle)
    return (
        jnp.concatenate([cosine, cosine], axis=1),
        jnp.concatenate([-sine, sine], axis=1),
    )


def turn(value, cosine, sine, straight):
    cosine = jnp.where(straight, 1.0, cosine)
    sine = jnp.where(straight, 0.0, sine)
    return value * cosine + pltpu.roll(value, HEAD_DIM // 2, 1) * sine


def params(mib):
    return pltpu.CompilerParams(vmem_limit_bytes=mib << 20)


def in_vmem(value):
    return pltpu.with_memory_space_constraint(value, pltpu.VMEM)


VMEM_SPEC = pl.BlockSpec(memory_space=pltpu.VMEM)
SMEM_SPEC = pl.BlockSpec(memory_space=pltpu.SMEM)
ANY_SPEC = pl.BlockSpec(memory_space=pl.ANY)


def over_weight(weight_ref, first, count, body):
    def step(at, carry):
        body(at, weight_ref[pl.ds(pl.multiple_of((first + at) * KBLK, KBLK), KBLK), :])
        return carry

    lax.fori_loop(0, count, step, 0)


def over_copied(weight_ref, buffer_ref, sem, count, body):
    def copy(at):
        rows = pl.ds(pl.multiple_of(at * KBLK, KBLK), KBLK)
        return pltpu.make_async_copy(weight_ref.at[rows, :], buffer_ref.at[at % 2], sem.at[at % 2])

    copy(0).start()

    def step(at, carry):
        @pl.when(at + 1 < count)
        def _():
            copy(at + 1).start()

        copy(at).wait()
        body(at, buffer_ref[at % 2])
        return carry

    lax.fori_loop(0, count, step, 0)


def product(over, low_ref, out_ref):
    def body(at, block):
        lanes = pl.ds(pl.multiple_of(at * KBLK, KBLK), KBLK)
        out_ref[:, lanes] = lax.dot_general(
            low_ref[...], block, (((1,), (1,)), ((), ())), preferred_element_type=jnp.float32
        )

    over(out_ref.shape[1] // KBLK, body)


def rotate_kernel(spots, grad_ref, cos_ref, sin_ref, weight_ref, out_ref, low_ref, bias_ref, *scratch):
    for head in range(grad_ref.shape[1] // HEAD_DIM):
        lanes = pl.ds(head * HEAD_DIM, HEAD_DIM)
        value = grad_ref[:, lanes].astype(jnp.float32)
        turned = turn(value, cos_ref[...], -sin_ref[...], spots[2 + head] == 1)
        bias_ref[:, lanes] = jnp.sum(turned, axis=0, keepdims=True)
        low_ref[:, lanes] = turned.astype(jnp.bfloat16)
    product(functools.partial(over_copied, weight_ref, *scratch), low_ref, out_ref)


def back_first(spots, grad, cosine, sine, weight):
    rows, cols = grad.shape
    return pl.pallas_call(
        rotate_kernel,
        in_specs=[SMEM_SPEC] + [VMEM_SPEC] * 3 + [ANY_SPEC],
        out_specs=[VMEM_SPEC] * 3,
        out_shape=[
            pltpu.VMEM((rows, weight.shape[0] // HALVES), jnp.float32),
            pltpu.VMEM((rows, cols), jnp.bfloat16),
            jax.ShapeDtypeStruct((1, cols), jnp.float32),
        ],
        scratch_shapes=[pltpu.VMEM((2, KBLK, cols), jnp.bfloat16), pltpu.SemaphoreType.DMA((2,))],
        compiler_params=params(6),
        name="back_first",
    )(spots, grad, cosine, sine, pltpu.with_memory_space_constraint(weight, pltpu.HBM))


def second_kernel(low_ref, weight_ref, out_ref):
    product(functools.partial(over_weight, weight_ref, out_ref.shape[1] // KBLK), low_ref, out_ref)


def back_second(low, weight):
    rows, _ = low.shape
    return pl.pallas_call(
        second_kernel,
        in_specs=[VMEM_SPEC] * 2,
        out_specs=VMEM_SPEC,
        out_shape=pltpu.VMEM((rows, weight.shape[0] // HALVES), jnp.float32),
        compiler_params=params(4),
        name="back_second",
    )(low, in_vmem(weight))


def over_columns(start, stop, body, block=CBLK):
    def step(at, carry):
        body(pl.multiple_of(start + at * block, block))
        return carry

    lax.fori_loop(0, (stop - start) // block, step, 0)


def away(spots, offset):
    return lax.rem(spots[0] + (offset + RING), RING)


def add_kernel(jobs, spots, first_ref, second_ref, *refs):
    half = first_ref.shape[1]
    arrived, outs = refs[: -len(jobs)], refs[-len(jobs) :]
    for (offset, (start, stop), taken), out_ref in zip(jobs, outs):
        rows = pl.ds(pl.multiple_of(away(spots, offset) * PAIR, PAIR), PAIR)
        spans = [span for _, span in taken]
        edges = {start, stop} | {e for span in ((half, half), *spans) for e in span if start < e < stop}
        edges = sorted(edges)
        for low, high in zip(edges[:-1], edges[1:]):
            source, base = (first_ref, 0) if low < half else (second_ref, half)
            adds = [(arrived[at], span[0]) for at, span in taken if span[0] <= low < span[1]]

            block = CBLK if (high - low) % CBLK == 0 else CBLK // 2

            def body(at):
                total = source[rows, pl.ds(at - base, block)]
                for ref, begin in adds:
                    total = total + ref[:, pl.ds(at - begin, block)].astype(jnp.float32)
                out_ref[:, pl.ds(at - start, block)] = total.astype(jnp.bfloat16)

            over_columns(low, high, body, block)


def added(spots, partials, jobs, arrived):
    return pl.pallas_call(
        functools.partial(add_kernel, jobs),
        in_specs=[SMEM_SPEC] + [VMEM_SPEC] * (2 + len(arrived)),
        out_specs=[VMEM_SPEC] * len(jobs),
        out_shape=[pltpu.VMEM((PAIR, stop - start), jnp.bfloat16) for _, (start, stop), _ in jobs],
        compiler_params=params(2),
        name="add",
    )(spots, *partials, *[in_vmem(value) for value in arrived])


def join_kernel(bounds, spots, first_ref, second_ref, rising_ref, falling_ref, mine_ref, other_ref):
    first, stop = bounds
    half = first_ref.shape[1]
    for at, out_ref in ((spots[1], mine_ref), (1 - spots[1], other_ref)):
        local = pl.ds(pl.multiple_of(at * TOK_DEV, TOK_DEV), TOK_DEV)
        whole = pl.ds(pl.multiple_of(spots[0] * PAIR + at * TOK_DEV, TOK_DEV), TOK_DEV)
        for source, low, high in ((first_ref, 0, half), (second_ref, half, 2 * half)):

            def body(start):
                lanes = pl.ds(start - first, CBLK)
                total = source[whole, pl.ds(start - low, CBLK)] + rising_ref[local, lanes].astype(jnp.float32)
                total = total + falling_ref[local, lanes].astype(jnp.float32)
                out_ref[:, lanes] = total.astype(out_ref.dtype)

            if max(first, low) < min(stop, high):
                over_columns(max(first, low), min(stop, high), body)


def joined(spots, partials, bounds, rising, falling):
    span = bounds[1] - bounds[0]
    return pl.pallas_call(
        functools.partial(join_kernel, bounds),
        in_specs=[SMEM_SPEC] + [VMEM_SPEC] * 4,
        out_specs=[VMEM_SPEC] * 2,
        out_shape=[
            pltpu.VMEM((TOK_DEV, span), jnp.float32),
            pltpu.VMEM((TOK_DEV, span), jnp.bfloat16),
        ],
        compiler_params=params(2),
        name="join",
    )(spots, *partials, in_vmem(rising), in_vmem(falling))


def sum_kernel(left_ref, right_ref, out_ref):
    out_ref[...] = left_ref[...] + right_ref[...]


def summed(left, right):
    return pl.pallas_call(
        sum_kernel,
        in_specs=[VMEM_SPEC] * 2,
        out_specs=VMEM_SPEC,
        out_shape=jax.ShapeDtypeStruct(left.shape, left.dtype),
        compiler_params=params(2),
        name="sum",
    )(left, right)


def finish_kernel(x_ref, gain_ref, mine0, other0, mine1, other1, left, right, out_ref, total_ref):
    total_ref[...] = left[...] + right[...]
    width = x_ref.shape[1]
    first = mine0.shape[1]
    squares = jnp.zeros((TOK_DEV, HEAD_DIM), jnp.float32)
    products = jnp.zeros((TOK_DEV, HEAD_DIM), jnp.float32)

    def at(start):
        mine, other, base = (mine0, other0, 0) if start < first else (mine1, other1, first)
        local = pl.ds(start - base, HEAD_DIM)
        grad = mine[:, local] + other[:, local].astype(jnp.float32)
        lanes = pl.ds(start, HEAD_DIM)
        return x_ref[:, lanes].astype(jnp.float32), gain_ref[:, lanes] * grad, lanes

    for start in range(0, width, HEAD_DIM):
        value, grad, _ = at(start)
        squares = squares + value * value
        products = products + grad * value
    scale = lax.rsqrt(jnp.sum(squares, axis=1, keepdims=True) / width + 1e-06)
    inner = scale * scale * scale * (jnp.sum(products, axis=1, keepdims=True) / width)
    for start in range(0, width, HEAD_DIM):
        value, grad, lanes = at(start)
        out_ref[:, lanes] = scale * grad - value * inner


def finished(tokens, gain, parts, sums):
    return pl.pallas_call(
        finish_kernel,
        out_shape=[
            jax.ShapeDtypeStruct(tokens.shape, jnp.float32),
            jax.ShapeDtypeStruct(gain.shape, jnp.float32),
        ],
        compiler_params=params(8),
        name="finish",
    )(tokens, gain, *parts, *sums)


def token_rows(spots, shift, swapped):
    side = 1 - spots[1] if swapped else spots[1]
    block = away(spots, shift) * (PAIR // TOK_DEV) + side
    return pl.ds(pl.multiple_of(block * TOK_DEV, TOK_DEV), TOK_DEV)


def norm_kernel(marks, spots, *refs):
    count = len(marks)
    xs, refs = refs[:count], refs[count:]
    first_ref, second_ref, gain_ref, refs = *refs[:3], refs[3:]
    normed_ref, total_ref = refs[-2:]
    width = gain_ref.shape[1]
    half = first_ref.shape[1]
    scales = []
    for j in range(count):

        def squares(at, total):
            for lane in range(0, CBLK, HEAD_DIM):
                lanes = pl.ds(pl.multiple_of(at * CBLK + lane, HEAD_DIM), HEAD_DIM)
                value = xs[j][:, lanes].astype(jnp.float32)
                total = total + value * value
            return total

        total = lax.fori_loop(0, width // CBLK, squares, jnp.zeros((TOK_DEV, HEAD_DIM), jnp.float32))
        scales.append(lax.rsqrt(jnp.sum(total, axis=1, keepdims=True) / width + 1e-06))

    for source, start in ((first_ref, 0), (second_ref, half)):

        def body(at):
            lanes = pl.ds(at, NBLK)
            gain = gain_ref[:, lanes]
            products = jnp.zeros((TOK_DEV, NBLK), jnp.float32)
            for j, mark in enumerate(marks):
                value = xs[j][:, lanes].astype(jnp.float32) * scales[j]
                products = products + source[token_rows(spots, *mark), pl.ds(at - start, NBLK)] * value
                normed_ref[j * TOK_DEV : (j + 1) * TOK_DEV, lanes] = (value * gain).astype(jnp.bfloat16)
            total = jnp.sum(products, axis=0, keepdims=True)
            if len(refs) > 2:
                total = total + refs[0][:, lanes]
            total_ref[:, lanes] = total

        over_columns(start, start + half, body, NBLK)


def normalized(marks, spots, pieces, partials, gain, carried):
    count = len(pieces)
    width = gain.shape[1]
    return pl.pallas_call(
        functools.partial(norm_kernel, marks),
        in_specs=[SMEM_SPEC] + [VMEM_SPEC] * (count + 3 + len(carried)),
        out_specs=[VMEM_SPEC] * 2,
        out_shape=[
            pltpu.VMEM((count * TOK_DEV, width), jnp.bfloat16),
            pltpu.VMEM((1, width), jnp.float32),
        ],
        compiler_params=params(2),
        name="norm",
    )(spots, *[in_vmem(piece) for piece in pieces], *partials, gain, *carried)


def project_kernel(marks, spots, *refs):
    groups = len(marks)
    normed, refs = refs[:groups], refs[groups:]
    weight_ref, bias_ref, cos_ref, sin_ref = refs[:4]
    out_ref, acc_ref, stage_ref, out_sem = refs[-4:]
    acc_ref[...] = jnp.zeros_like(acc_ref)

    def body(at, block):
        lanes = pl.ds(pl.multiple_of(at * KBLK, KBLK), KBLK)
        values = [ref[:, lanes] for ref in normed]
        value = values[0] if groups == 1 else jnp.concatenate(values, axis=0)
        acc_ref[...] += jnp.dot(value, block, preferred_element_type=jnp.float32)

    over_weight(weight_ref, 0, weight_ref.shape[0] // KBLK, body)
    copies = []
    for j, mark in enumerate(mark for group in marks for mark in group):
        rows = pl.ds(j * TOK_DEV, TOK_DEV)
        whole = token_rows(spots, *mark)
        for head in range(stage_ref.shape[1] // HEAD_DIM):
            lanes = pl.ds(head * HEAD_DIM, HEAD_DIM)
            value = acc_ref[rows, lanes] + bias_ref[:, lanes]
            stage_ref[rows, lanes] = turn(
                value, cos_ref[whole, :], sin_ref[whole, :], spots[2 + head] == 1
            ).astype(jnp.bfloat16)
        copy = pltpu.make_async_copy(stage_ref.at[rows, :], out_ref.at[whole, :], out_sem.at[j])
        copy.start()
        copies.append(copy)
    for copy in copies:
        copy.wait()


def project(marks, spots, normed, weight, bias, cosine, sine, carried):
    rows, cols = sum(part.shape[0] for part in normed), weight.shape[1]
    in_specs = [SMEM_SPEC] + [VMEM_SPEC] * (len(normed) + 4)
    return pl.pallas_call(
        functools.partial(project_kernel, marks),
        in_specs=in_specs + [ANY_SPEC] * len(carried),
        out_specs=ANY_SPEC,
        out_shape=pltpu.HBM((cosine.shape[0], cols), jnp.bfloat16),
        scratch_shapes=[
            pltpu.VMEM((rows, cols), jnp.float32),
            pltpu.VMEM((rows, cols), jnp.bfloat16),
            pltpu.SemaphoreType.DMA((rows // TOK_DEV,)),
        ],
        input_output_aliases={len(in_specs): 0} if carried else {},
        compiler_params=params(4),
        name="project",
    )(spots, *normed, in_vmem(weight), bias, cosine, sine, *carried)


def work(tokens, norm_gain, qkv_weight, qkv_bias, qkv_grad):
    width, cols = qkv_weight.shape
    rows = qkv_grad.shape[0]
    heads = cols // HEAD_DIM
    ring = lax.axis_index("mp_0")
    side = lax.axis_index("mp_1")
    first_head = lax.axis_index(MP) * heads
    straight = ((first_head + jnp.arange(heads)) % GROUP == GROUP - 1).astype(jnp.int32)
    spots = jnp.concatenate([jnp.stack([ring, side]).astype(jnp.int32), straight])
    cosine, sine = tables(rows, SEQ_LEN // lax.axis_size(MP))
    bias_row = qkv_bias[None, :]
    spots, cosine, sine, gain_row, bias_row, qkv_grad = lax.optimization_barrier(
        (spots, cosine, sine, norm_gain[None, :], bias_row, qkv_grad)
    )
    cosine, sine, gain_row, bias_row = map(in_vmem, (cosine, sine, gain_row, bias_row))

    ups, downs = [tokens], [tokens]
    for _ in range(1, RING // 2 + 1):
        ups.append(up(ups[-1]))
    for _ in range(1, RING // 2):
        downs.append(down(downs[-1]))
    near = {"0": (0, tokens, swap(tokens))}
    for step in range(1, RING // 2 + 1):
        near[f"{step}u"] = (-step, ups[step], swap(ups[step]))
        if step < RING // 2:
            near[f"{step}d"] = (step, downs[step], swap(downs[step]))

    first, low, bias_grad = back_first(spots, qkv_grad, cosine, sine, qkv_weight)
    partials = (in_vmem(first), in_vmem(back_second(low, qkv_weight)))

    half = width // HALVES
    cut_a, cut_b, rest = (0, CUT), (CUT, width), (half, width)
    far_u, far_d = (0, UP_FAR), (UP_FAR, half)
    early = partials[:1] * 2

    def taken(at, span):
        return ((at, span),)

    rising, falling = added(spots, early, ((4, far_u, ()), (-4, far_d, ())), ())
    up4, down4a = up(rising), down(falling)
    (falling,) = added(spots, partials, ((-4, rest, ()),), ())
    down4b = down(falling)
    (rising,) = added(spots, partials, ((3, cut_a, taken(0, far_u)),), (up4,))
    up3a = up(rising)
    rising, falling = added(
        spots, partials, ((3, cut_b, ()), (-3, cut_a, taken(0, far_d) + taken(1, rest))), (down4a, down4b)
    )
    up3b, down3a = up(rising), down(falling)
    (falling,) = added(spots, partials, ((-3, cut_b, taken(0, rest)),), (down4b,))
    down3b = down(falling)
    rising, falling, later = added(
        spots,
        partials,
        ((2, cut_a, taken(0, cut_a)), (-2, cut_a, taken(1, cut_a)), (2, cut_b, taken(2, cut_b))),
        (up3a, down3a, up3b),
    )
    up2a, down2a, up2b = up(rising), down(falling), up(later)
    (falling,) = added(spots, partials, ((-2, cut_b, taken(0, cut_b)),), (down3b,))
    down2b = down(falling)
    parts = []
    for span, rising, falling in ((cut_a, up2a, down2a), (cut_b, up2b, down2b)):
        rising, falling = added(
            spots, partials, ((1, span, taken(0, span)), (-1, span, taken(1, span))), (rising, falling)
        )
        rising, falling = up(rising), down(falling)
        mine, other = joined(spots, partials, span, rising, falling)
        parts += [mine, swap(other)]

    sums, batches = (), []
    for names in (("0", "1u"), ("1d", "2u"), ("2d", "3u"), ("3d", "4u")):
        group = [near[name] for name in names]
        pieces = [piece for _, piece, _ in group] + [piece for _, _, piece in group]
        marks = tuple((shift, swapped) for swapped in (False, True) for shift, _, _ in group)
        normed, total = normalized(marks, spots, pieces, partials, gain_row, sums)
        sums = (total,)
        batches.append((marks, normed))
    out = ()
    for batch in (batches[:1], batches[1:2], batches[2:3], batches[3:]):
        marks, normed = zip(*batch)
        out = (
            project(marks, spots, normed, qkv_weight, bias_row, cosine, sine, out),
        )

    total = summed(total, swap(total))
    for reach in (4, 1, 2):
        pairs = [(i, i ^ reach) for i in range(RING)]
        sums = (total, lax.ppermute(total, "mp_0", pairs))
        if reach != 2:
            total = summed(*sums)

    bias_grad, parts[2] = lax.optimization_barrier((bias_grad, parts[2]))
    tokens_grad, total = finished(tokens, gain_row, parts, sums)
    return (out[0], tokens_grad, total[0], bias_grad[0])


def solution(mesh):
    split = Mesh(mesh.devices.reshape(mesh.shape["dp"], 8, 2), ("dp", "mp_0", "mp_1"))
    placed = (P(DP_MP, None), P(), P(None, MP), P(MP), P("dp", MP))
    return jax.shard_map(
        work,
        mesh=split,
        in_specs=placed,
        out_specs=(P("dp", MP), P(DP_MP, None), P("dp"), P(DP_MP)),
        check_vma=False,
    )
```

```python
import functools

import jax
import jax.numpy as jnp
from jax import lax
from jax.experimental import pallas as pl
from jax.experimental.pallas import tpu as pltpu
from jax.sharding import Mesh
from jax.sharding import PartitionSpec as P

HEAD_DIM = 128
SEQ_LEN = 32768
GROUP = 10
TOK_DEV = 32
PAIR = 2 * TOK_DEV
RING = 8
MP = ("mp_0", "mp_1")
DP_MP = ("dp", "mp_0", "mp_1")
UP = [(i, (i + 1) % RING) for i in range(RING)]
DOWN = [(i, (i - 1) % RING) for i in range(RING)]
SWAP = [(0, 1), (1, 0)]
KBLK = 1024
FIRST = 3072
CBLK = 512
NBLK = 256
UP_FAR = 2048
CUT = 5120


def up(value):
    return lax.ppermute(value, "mp_0", UP)


def down(value):
    return lax.ppermute(value, "mp_0", DOWN)


def swap(value):
    return lax.ppermute(value, "mp_1", SWAP)


def tables(rows, stride):
    half = HEAD_DIM // 2
    row_index = jnp.arange(rows)
    place = row_index // TOK_DEV * stride + row_index % TOK_DEV
    inverse = jnp.exp(
        -jnp.log(jnp.float32(1000000.0)) * (2.0 * jnp.arange(half).astype(jnp.float32) / HEAD_DIM)
    )
    angle = place.astype(jnp.float32)[:, None] * inverse[None, :]
    cosine, sine = jnp.cos(angle), jnp.sin(angle)
    return (
        jnp.concatenate([cosine, cosine], axis=1),
        jnp.concatenate([-sine, sine], axis=1),
    )


def turn(value, cosine, sine, straight):
    cosine = jnp.where(straight, 1.0, cosine)
    sine = jnp.where(straight, 0.0, sine)
    return value * cosine + pltpu.roll(value, HEAD_DIM // 2, 1) * sine


def params(mib):
    return pltpu.CompilerParams(vmem_limit_bytes=mib << 20)


def in_vmem(value):
    return pltpu.with_memory_space_constraint(value, pltpu.VMEM)


VMEM_SPEC = pl.BlockSpec(memory_space=pltpu.VMEM)
SMEM_SPEC = pl.BlockSpec(memory_space=pltpu.SMEM)
ANY_SPEC = pl.BlockSpec(memory_space=pl.ANY)


def over_weight(weight_ref, first, count, body):
    def step(at, carry):
        body(at, weight_ref[pl.ds(pl.multiple_of((first + at) * KBLK, KBLK), KBLK), :])
        return carry

    lax.fori_loop(0, count, step, 0)


def over_copied(weight_ref, buffer_ref, sem, count, body):
    def copy(at):
        rows = pl.ds(pl.multiple_of(at * KBLK, KBLK), KBLK)
        return pltpu.make_async_copy(weight_ref.at[rows, :], buffer_ref.at[at % 2], sem.at[at % 2])

    copy(0).start()

    def step(at, carry):
        @pl.when(at + 1 < count)
        def _():
            copy(at + 1).start()

        copy(at).wait()
        body(at, buffer_ref[at % 2])
        return carry

    lax.fori_loop(0, count, step, 0)


def product(over, low_ref, out_ref):
    def body(at, block):
        lanes = pl.ds(pl.multiple_of(at * KBLK, KBLK), KBLK)
        out_ref[:, lanes] = lax.dot_general(
            low_ref[...], block, (((1,), (1,)), ((), ())), preferred_element_type=jnp.float32
        )

    over(out_ref.shape[1] // KBLK, body)


def rotate_kernel(spots, grad_ref, cos_ref, sin_ref, weight_ref, out_ref, low_ref, bias_ref, *scratch):
    for head in range(grad_ref.shape[1] // HEAD_DIM):
        lanes = pl.ds(head * HEAD_DIM, HEAD_DIM)
        value = grad_ref[:, lanes].astype(jnp.float32)
        turned = turn(value, cos_ref[...], -sin_ref[...], spots[2 + head] == 1)
        bias_ref[:, lanes] = jnp.sum(turned, axis=0, keepdims=True)
        low_ref[:, lanes] = turned.astype(jnp.bfloat16)
    product(functools.partial(over_copied, weight_ref, *scratch), low_ref, out_ref)


def back_first(spots, grad, cosine, sine, weight):
    rows, cols = grad.shape
    return pl.pallas_call(
        rotate_kernel,
        in_specs=[SMEM_SPEC] + [VMEM_SPEC] * 3 + [ANY_SPEC],
        out_specs=[VMEM_SPEC] * 3,
        out_shape=[
            pltpu.VMEM((rows, FIRST), jnp.float32),
            pltpu.VMEM((rows, cols), jnp.bfloat16),
            jax.ShapeDtypeStruct((1, cols), jnp.float32),
        ],
        scratch_shapes=[pltpu.VMEM((2, KBLK, cols), jnp.bfloat16), pltpu.SemaphoreType.DMA((2,))],
        compiler_params=params(6),
        name="back_first",
    )(spots, grad, cosine, sine, pltpu.with_memory_space_constraint(weight, pltpu.HBM))


def second_kernel(low_ref, weight_ref, out_ref):
    product(functools.partial(over_weight, weight_ref, FIRST // KBLK), low_ref, out_ref)


def back_second(low, weight):
    rows, _ = low.shape
    return pl.pallas_call(
        second_kernel,
        in_specs=[VMEM_SPEC] * 2,
        out_specs=VMEM_SPEC,
        out_shape=pltpu.VMEM((rows, weight.shape[0] - FIRST), jnp.float32),
        compiler_params=params(4),
        name="back_second",
    )(low, in_vmem(weight))


def over_columns(start, stop, body, block=CBLK):
    def step(at, carry):
        body(pl.multiple_of(start + at * block, block))
        return carry

    lax.fori_loop(0, (stop - start) // block, step, 0)


def away(spots, offset):
    return lax.rem(spots[0] + (offset + RING), RING)


def add_kernel(jobs, spots, first_ref, second_ref, *refs):
    half = first_ref.shape[1]
    arrived, outs = refs[: -len(jobs)], refs[-len(jobs) :]
    for (offset, (start, stop), taken), out_ref in zip(jobs, outs):
        rows = pl.ds(pl.multiple_of(away(spots, offset) * PAIR, PAIR), PAIR)
        spans = [span for _, span in taken]
        edges = {start, stop} | {e for span in ((half, half), *spans) for e in span if start < e < stop}
        edges = sorted(edges)
        for low, high in zip(edges[:-1], edges[1:]):
            source, base = (first_ref, 0) if low < half else (second_ref, half)
            adds = [(arrived[at], span[0]) for at, span in taken if span[0] <= low < span[1]]

            block = CBLK if (high - low) % CBLK == 0 else CBLK // 2

            def body(at):
                total = source[rows, pl.ds(at - base, block)]
                for ref, begin in adds:
                    total = total + ref[:, pl.ds(at - begin, block)].astype(jnp.float32)
                out_ref[:, pl.ds(at - start, block)] = total.astype(jnp.bfloat16)

            over_columns(low, high, body, block)


def added(spots, partials, jobs, arrived):
    return pl.pallas_call(
        functools.partial(add_kernel, jobs),
        in_specs=[SMEM_SPEC] + [VMEM_SPEC] * (2 + len(arrived)),
        out_specs=[VMEM_SPEC] * len(jobs),
        out_shape=[pltpu.VMEM((PAIR, stop - start), jnp.bfloat16) for _, (start, stop), _ in jobs],
        compiler_params=params(2),
        name="add",
    )(spots, *partials, *[in_vmem(value) for value in arrived])


def join_kernel(bounds, spots, first_ref, second_ref, rising_ref, falling_ref, mine_ref, other_ref):
    first, stop = bounds
    half = first_ref.shape[1]
    for at, out_ref in ((spots[1], mine_ref), (1 - spots[1], other_ref)):
        local = pl.ds(pl.multiple_of(at * TOK_DEV, TOK_DEV), TOK_DEV)
        whole = pl.ds(pl.multiple_of(spots[0] * PAIR + at * TOK_DEV, TOK_DEV), TOK_DEV)
        for source, low, high in ((first_ref, 0, half), (second_ref, half, half + second_ref.shape[1])):

            def body(start):
                lanes = pl.ds(start - first, CBLK)
                total = source[whole, pl.ds(start - low, CBLK)] + rising_ref[local, lanes].astype(jnp.float32)
                total = total + falling_ref[local, lanes].astype(jnp.float32)
                out_ref[:, lanes] = total.astype(out_ref.dtype)

            if max(first, low) < min(stop, high):
                over_columns(max(first, low), min(stop, high), body)


def joined(spots, partials, bounds, rising, falling):
    span = bounds[1] - bounds[0]
    return pl.pallas_call(
        functools.partial(join_kernel, bounds),
        in_specs=[SMEM_SPEC] + [VMEM_SPEC] * 4,
        out_specs=[VMEM_SPEC] * 2,
        out_shape=[
            pltpu.VMEM((TOK_DEV, span), jnp.float32),
            pltpu.VMEM((TOK_DEV, span), jnp.bfloat16),
        ],
        compiler_params=params(2),
        name="join",
    )(spots, *partials, in_vmem(rising), in_vmem(falling))


def sum_kernel(left_ref, right_ref, out_ref):
    out_ref[...] = left_ref[...] + right_ref[...]


def summed(left, right):
    return pl.pallas_call(
        sum_kernel,
        in_specs=[VMEM_SPEC] * 2,
        out_specs=VMEM_SPEC,
        out_shape=jax.ShapeDtypeStruct(left.shape, left.dtype),
        compiler_params=params(2),
        name="sum",
    )(left, right)


def finish_kernel(x_ref, gain_ref, mine0, other0, mine1, other1, left, right, out_ref, total_ref):
    total_ref[...] = left[...] + right[...]
    width = x_ref.shape[1]
    first = mine0.shape[1]
    squares = jnp.zeros((TOK_DEV, HEAD_DIM), jnp.float32)
    products = jnp.zeros((TOK_DEV, HEAD_DIM), jnp.float32)

    def at(start):
        mine, other, base = (mine0, other0, 0) if start < first else (mine1, other1, first)
        local = pl.ds(start - base, HEAD_DIM)
        grad = mine[:, local] + other[:, local].astype(jnp.float32)
        lanes = pl.ds(start, HEAD_DIM)
        return x_ref[:, lanes].astype(jnp.float32), gain_ref[:, lanes] * grad, lanes

    for start in range(0, width, HEAD_DIM):
        value, grad, _ = at(start)
        squares = squares + value * value
        products = products + grad * value
    scale = lax.rsqrt(jnp.sum(squares, axis=1, keepdims=True) / width + 1e-06)
    inner = scale * scale * scale * (jnp.sum(products, axis=1, keepdims=True) / width)
    for start in range(0, width, HEAD_DIM):
        value, grad, lanes = at(start)
        out_ref[:, lanes] = scale * grad - value * inner


def finished(tokens, gain, parts, sums):
    return pl.pallas_call(
        finish_kernel,
        out_shape=[
            jax.ShapeDtypeStruct(tokens.shape, jnp.float32),
            jax.ShapeDtypeStruct(gain.shape, jnp.float32),
        ],
        compiler_params=params(8),
        name="finish",
    )(tokens, gain, *parts, *sums)


def token_rows(spots, shift, swapped):
    side = 1 - spots[1] if swapped else spots[1]
    block = away(spots, shift) * (PAIR // TOK_DEV) + side
    return pl.ds(pl.multiple_of(block * TOK_DEV, TOK_DEV), TOK_DEV)


def norm_kernel(marks, spots, *refs):
    count = len(marks)
    xs, refs = refs[:count], refs[count:]
    first_ref, second_ref, gain_ref, refs = *refs[:3], refs[3:]
    normed_ref, total_ref = refs[-2:]
    width = gain_ref.shape[1]
    half = first_ref.shape[1]
    scales = []
    for j in range(count):

        def squares(at, total):
            for lane in range(0, CBLK, HEAD_DIM):
                lanes = pl.ds(pl.multiple_of(at * CBLK + lane, HEAD_DIM), HEAD_DIM)
                value = xs[j][:, lanes].astype(jnp.float32)
                total = total + value * value
            return total

        total = lax.fori_loop(0, width // CBLK, squares, jnp.zeros((TOK_DEV, HEAD_DIM), jnp.float32))
        scales.append(lax.rsqrt(jnp.sum(total, axis=1, keepdims=True) / width + 1e-06))

    for source, start in ((first_ref, 0), (second_ref, half)):

        def body(at):
            lanes = pl.ds(at, NBLK)
            gain = gain_ref[:, lanes]
            products = jnp.zeros((TOK_DEV, NBLK), jnp.float32)
            for j, mark in enumerate(marks):
                value = xs[j][:, lanes].astype(jnp.float32) * scales[j]
                products = products + source[token_rows(spots, *mark), pl.ds(at - start, NBLK)] * value
                normed_ref[j * TOK_DEV : (j + 1) * TOK_DEV, lanes] = (value * gain).astype(jnp.bfloat16)
            total = jnp.sum(products, axis=0, keepdims=True)
            if len(refs) > 2:
                total = total + refs[0][:, lanes]
            total_ref[:, lanes] = total

        over_columns(start, start + source.shape[1], body, NBLK)


def normalized(marks, spots, pieces, partials, gain, carried):
    count = len(pieces)
    width = gain.shape[1]
    return pl.pallas_call(
        functools.partial(norm_kernel, marks),
        in_specs=[SMEM_SPEC] + [VMEM_SPEC] * (count + 3 + len(carried)),
        out_specs=[VMEM_SPEC] * 2,
        out_shape=[
            pltpu.VMEM((count * TOK_DEV, width), jnp.bfloat16),
            pltpu.VMEM((1, width), jnp.float32),
        ],
        compiler_params=params(2),
        name="norm",
    )(spots, *[in_vmem(piece) for piece in pieces], *partials, gain, *carried)


def project_kernel(marks, spots, *refs):
    groups = len(marks)
    normed, refs = refs[:groups], refs[groups:]
    weight_ref, bias_ref, cos_ref, sin_ref = refs[:4]
    out_ref, acc_ref, stage_ref, out_sem = refs[-4:]
    acc_ref[...] = jnp.zeros_like(acc_ref)

    def body(at, block):
        lanes = pl.ds(pl.multiple_of(at * KBLK, KBLK), KBLK)
        values = [ref[:, lanes] for ref in normed]
        value = values[0] if groups == 1 else jnp.concatenate(values, axis=0)
        acc_ref[...] += jnp.dot(value, block, preferred_element_type=jnp.float32)

    over_weight(weight_ref, 0, weight_ref.shape[0] // KBLK, body)
    copies = []
    for j, mark in enumerate(mark for group in marks for mark in group):
        rows = pl.ds(j * TOK_DEV, TOK_DEV)
        whole = token_rows(spots, *mark)
        for head in range(stage_ref.shape[1] // HEAD_DIM):
            lanes = pl.ds(head * HEAD_DIM, HEAD_DIM)
            value = acc_ref[rows, lanes] + bias_ref[:, lanes]
            stage_ref[rows, lanes] = turn(
                value, cos_ref[whole, :], sin_ref[whole, :], spots[2 + head] == 1
            ).astype(jnp.bfloat16)
        copy = pltpu.make_async_copy(stage_ref.at[rows, :], out_ref.at[whole, :], out_sem.at[j])
        copy.start()
        copies.append(copy)
    for copy in copies:
        copy.wait()


def project(marks, spots, normed, weight, bias, cosine, sine, carried):
    rows, cols = sum(part.shape[0] for part in normed), weight.shape[1]
    in_specs = [SMEM_SPEC] + [VMEM_SPEC] * (len(normed) + 4)
    return pl.pallas_call(
        functools.partial(project_kernel, marks),
        in_specs=in_specs + [ANY_SPEC] * len(carried),
        out_specs=ANY_SPEC,
        out_shape=pltpu.HBM((cosine.shape[0], cols), jnp.bfloat16),
        scratch_shapes=[
            pltpu.VMEM((rows, cols), jnp.float32),
            pltpu.VMEM((rows, cols), jnp.bfloat16),
            pltpu.SemaphoreType.DMA((rows // TOK_DEV,)),
        ],
        input_output_aliases={len(in_specs): 0} if carried else {},
        compiler_params=params(4),
        name="project",
    )(spots, *normed, in_vmem(weight), bias, cosine, sine, *carried)


def work(tokens, norm_gain, qkv_weight, qkv_bias, qkv_grad):
    width, cols = qkv_weight.shape
    rows = qkv_grad.shape[0]
    heads = cols // HEAD_DIM
    ring = lax.axis_index("mp_0")
    side = lax.axis_index("mp_1")
    first_head = lax.axis_index(MP) * heads
    straight = ((first_head + jnp.arange(heads)) % GROUP == GROUP - 1).astype(jnp.int32)
    spots = jnp.concatenate([jnp.stack([ring, side]).astype(jnp.int32), straight])
    cosine, sine = tables(rows, SEQ_LEN // lax.axis_size(MP))
    bias_row = qkv_bias[None, :]
    spots, cosine, sine, gain_row, bias_row, qkv_grad = lax.optimization_barrier(
        (spots, cosine, sine, norm_gain[None, :], bias_row, qkv_grad)
    )
    cosine, sine, gain_row, bias_row = map(in_vmem, (cosine, sine, gain_row, bias_row))

    ups, downs = [tokens], [tokens]
    for _ in range(1, RING // 2 + 1):
        ups.append(up(ups[-1]))
    for _ in range(1, RING // 2):
        downs.append(down(downs[-1]))
    near = {"0": (0, tokens, swap(tokens))}
    for step in range(1, RING // 2 + 1):
        near[f"{step}u"] = (-step, ups[step], swap(ups[step]))
        if step < RING // 2:
            near[f"{step}d"] = (step, downs[step], swap(downs[step]))

    first, low, bias_grad = back_first(spots, qkv_grad, cosine, sine, qkv_weight)
    partials = (in_vmem(first), in_vmem(back_second(low, qkv_weight)))

    cut_a, cut_b, rest = (0, CUT), (CUT, width), (FIRST, width)
    far_u, far_d = (0, UP_FAR), (UP_FAR, FIRST)
    early = partials[:1] * 2

    def taken(at, span):
        return ((at, span),)

    rising, falling = added(spots, early, ((4, far_u, ()), (-4, far_d, ())), ())
    up4, down4a = up(rising), down(falling)
    (falling,) = added(spots, partials, ((-4, rest, ()),), ())
    down4b = down(falling)
    (rising,) = added(spots, partials, ((3, cut_a, taken(0, far_u)),), (up4,))
    up3a = up(rising)
    rising, falling = added(
        spots, partials, ((3, cut_b, ()), (-3, cut_a, taken(0, far_d) + taken(1, rest))), (down4a, down4b)
    )
    up3b, down3a = up(rising), down(falling)
    (falling,) = added(spots, partials, ((-3, cut_b, taken(0, rest)),), (down4b,))
    down3b = down(falling)
    rising, falling, later = added(
        spots,
        partials,
        ((2, cut_a, taken(0, cut_a)), (-2, cut_a, taken(1, cut_a)), (2, cut_b, taken(2, cut_b))),
        (up3a, down3a, up3b),
    )
    up2a, down2a, up2b = up(rising), down(falling), up(later)
    (falling,) = added(spots, partials, ((-2, cut_b, taken(0, cut_b)),), (down3b,))
    down2b = down(falling)
    parts = []
    for span, rising, falling in ((cut_a, up2a, down2a), (cut_b, up2b, down2b)):
        rising, falling = added(
            spots, partials, ((1, span, taken(0, span)), (-1, span, taken(1, span))), (rising, falling)
        )
        rising, falling = up(rising), down(falling)
        mine, other = joined(spots, partials, span, rising, falling)
        parts += [mine, swap(other)]

    sums, batches = (), []
    for names in (("0", "1u"), ("1d", "2u"), ("2d", "3u"), ("3d", "4u")):
        group = [near[name] for name in names]
        pieces = [piece for _, piece, _ in group] + [piece for _, _, piece in group]
        marks = tuple((shift, swapped) for swapped in (False, True) for shift, _, _ in group)
        normed, total = normalized(marks, spots, pieces, partials, gain_row, sums)
        sums = (total,)
        batches.append((marks, normed))
    out = ()
    for batch in (batches[:1], batches[1:2], batches[2:3], batches[3:]):
        marks, normed = zip(*batch)
        out = (
            project(marks, spots, normed, qkv_weight, bias_row, cosine, sine, out),
        )

    total = summed(total, swap(total))
    for reach in (4, 2, 1):
        pairs = [(i, i ^ reach) for i in range(RING)]
        sums = (total, lax.ppermute(total, "mp_0", pairs))
        if reach != 1:
            total = summed(*sums)

    bias_grad, parts[2] = lax.optimization_barrier((bias_grad, parts[2]))
    tokens_grad, total = finished(tokens, gain_row, parts, sums)
    return (out[0], tokens_grad, total[0], bias_grad[0])


def solution(mesh):
    split = Mesh(mesh.devices.reshape(mesh.shape["dp"], 8, 2), ("dp", "mp_0", "mp_1"))
    placed = (P(DP_MP, None), P(), P(None, MP), P(MP), P("dp", MP))
    return jax.shard_map(
        work,
        mesh=split,
        in_specs=placed,
        out_specs=(P("dp", MP), P(DP_MP, None), P("dp"), P(DP_MP)),
        check_vma=False,
    )
```

```python
import functools

import jax
import jax.numpy as jnp
from jax import lax
from jax.experimental import pallas as pl
from jax.experimental.pallas import tpu as pltpu
from jax.sharding import Mesh
from jax.sharding import PartitionSpec as P

HEAD_DIM = 128
SEQ_LEN = 32768
GROUP = 10
TOK_DEV = 32
PAIR = 2 * TOK_DEV
RING = 8
MP = ("mp_0", "mp_1")
DP_MP = ("dp", "mp_0", "mp_1")
UP = [(i, (i + 1) % RING) for i in range(RING)]
DOWN = [(i, (i - 1) % RING) for i in range(RING)]
SWAP = [(0, 1), (1, 0)]
KBLK = 1024
FIRST = 3072
CBLK = 512
NBLK = 256
UP_FAR = 2048
CUT = 5120


def up(value):
    return lax.ppermute(value, "mp_0", UP)


def down(value):
    return lax.ppermute(value, "mp_0", DOWN)


def swap(value):
    return lax.ppermute(value, "mp_1", SWAP)


def tables(rows, stride):
    half = HEAD_DIM // 2
    row_index = jnp.arange(rows)
    place = row_index // TOK_DEV * stride + row_index % TOK_DEV
    inverse = jnp.exp(
        -jnp.log(jnp.float32(1000000.0)) * (2.0 * jnp.arange(half).astype(jnp.float32) / HEAD_DIM)
    )
    angle = place.astype(jnp.float32)[:, None] * inverse[None, :]
    cosine, sine = jnp.cos(angle), jnp.sin(angle)
    return (
        jnp.concatenate([cosine, cosine], axis=1),
        jnp.concatenate([-sine, sine], axis=1),
    )


def turn(value, cosine, sine, straight):
    cosine = jnp.where(straight, 1.0, cosine)
    sine = jnp.where(straight, 0.0, sine)
    return value * cosine + pltpu.roll(value, HEAD_DIM // 2, 1) * sine


def params(mib):
    return pltpu.CompilerParams(vmem_limit_bytes=mib << 20)


def in_vmem(value):
    return pltpu.with_memory_space_constraint(value, pltpu.VMEM)


VMEM_SPEC = pl.BlockSpec(memory_space=pltpu.VMEM)
SMEM_SPEC = pl.BlockSpec(memory_space=pltpu.SMEM)
ANY_SPEC = pl.BlockSpec(memory_space=pl.ANY)


def over_weight(weight_ref, first, count, body):
    def step(at, carry):
        body(at, weight_ref[pl.ds(pl.multiple_of((first + at) * KBLK, KBLK), KBLK), :])
        return carry

    lax.fori_loop(0, count, step, 0)


def over_copied(weight_ref, buffer_ref, sem, count, body):
    def copy(at):
        rows = pl.ds(pl.multiple_of(at * KBLK, KBLK), KBLK)
        return pltpu.make_async_copy(weight_ref.at[rows, :], buffer_ref.at[at % 2], sem.at[at % 2])

    copy(0).start()

    def step(at, carry):
        @pl.when(at + 1 < count)
        def _():
            copy(at + 1).start()

        copy(at).wait()
        body(at, buffer_ref[at % 2])
        return carry

    lax.fori_loop(0, count, step, 0)


def product(over, low_ref, out_ref):
    def body(at, block):
        lanes = pl.ds(pl.multiple_of(at * KBLK, KBLK), KBLK)
        out_ref[:, lanes] = lax.dot_general(
            low_ref[...], block, (((1,), (1,)), ((), ())), preferred_element_type=jnp.float32
        )

    over(out_ref.shape[1] // KBLK, body)


def rotate_kernel(spots, grad_ref, cos_ref, sin_ref, weight_ref, out_ref, low_ref, bias_ref, *scratch):
    for head in range(grad_ref.shape[1] // HEAD_DIM):
        lanes = pl.ds(head * HEAD_DIM, HEAD_DIM)
        value = grad_ref[:, lanes].astype(jnp.float32)
        turned = turn(value, cos_ref[...], -sin_ref[...], spots[2 + head] == 1)
        bias_ref[:, lanes] = jnp.sum(turned, axis=0, keepdims=True)
        low_ref[:, lanes] = turned.astype(jnp.bfloat16)
    product(functools.partial(over_copied, weight_ref, *scratch), low_ref, out_ref)


def back_first(spots, grad, cosine, sine, weight):
    rows, cols = grad.shape
    return pl.pallas_call(
        rotate_kernel,
        in_specs=[SMEM_SPEC] + [VMEM_SPEC] * 3 + [ANY_SPEC],
        out_specs=[VMEM_SPEC] * 3,
        out_shape=[
            pltpu.VMEM((rows, FIRST), jnp.float32),
            pltpu.VMEM((rows, cols), jnp.bfloat16),
            jax.ShapeDtypeStruct((1, cols), jnp.float32),
        ],
        scratch_shapes=[pltpu.VMEM((2, KBLK, cols), jnp.bfloat16), pltpu.SemaphoreType.DMA((2,))],
        compiler_params=params(6),
        name="back_first",
    )(spots, grad, cosine, sine, pltpu.with_memory_space_constraint(weight, pltpu.HBM))


def second_kernel(low_ref, weight_ref, out_ref):
    product(functools.partial(over_weight, weight_ref, FIRST // KBLK), low_ref, out_ref)


def back_second(low, weight):
    rows, _ = low.shape
    return pl.pallas_call(
        second_kernel,
        in_specs=[VMEM_SPEC] * 2,
        out_specs=VMEM_SPEC,
        out_shape=pltpu.VMEM((rows, weight.shape[0] - FIRST), jnp.float32),
        compiler_params=params(4),
        name="back_second",
    )(low, in_vmem(weight))


def over_columns(start, stop, body, block=CBLK):
    def step(at, carry):
        body(pl.multiple_of(start + at * block, block))
        return carry

    lax.fori_loop(0, (stop - start) // block, step, 0)


def away(spots, offset):
    return lax.rem(spots[0] + (offset + RING), RING)


def add_kernel(jobs, spots, first_ref, second_ref, *refs):
    half = first_ref.shape[1]
    arrived, outs = refs[: -len(jobs)], refs[-len(jobs) :]
    for (offset, (start, stop), taken), out_ref in zip(jobs, outs):
        rows = pl.ds(pl.multiple_of(away(spots, offset) * PAIR, PAIR), PAIR)
        spans = [span for _, span in taken]
        edges = {start, stop} | {e for span in ((half, half), *spans) for e in span if start < e < stop}
        edges = sorted(edges)
        for low, high in zip(edges[:-1], edges[1:]):
            source, base = (first_ref, 0) if low < half else (second_ref, half)
            adds = [(arrived[at], span[0]) for at, span in taken if span[0] <= low < span[1]]

            block = CBLK if (high - low) % CBLK == 0 else CBLK // 2

            def body(at):
                total = source[rows, pl.ds(at - base, block)]
                for ref, begin in adds:
                    total = total + ref[:, pl.ds(at - begin, block)].astype(jnp.float32)
                out_ref[:, pl.ds(at - start, block)] = total.astype(jnp.bfloat16)

            over_columns(low, high, body, block)


def added(spots, partials, jobs, arrived):
    return pl.pallas_call(
        functools.partial(add_kernel, jobs),
        in_specs=[SMEM_SPEC] + [VMEM_SPEC] * (2 + len(arrived)),
        out_specs=[VMEM_SPEC] * len(jobs),
        out_shape=[pltpu.VMEM((PAIR, stop - start), jnp.bfloat16) for _, (start, stop), _ in jobs],
        compiler_params=params(2),
        name="add",
    )(spots, *partials, *[in_vmem(value) for value in arrived])


def join_kernel(bounds, swapped, spots, first_ref, second_ref, rising_ref, falling_ref, out_ref):
    first, stop = bounds
    half = first_ref.shape[1]
    at = 1 - spots[1] if swapped else spots[1]
    local = pl.ds(pl.multiple_of(at * TOK_DEV, TOK_DEV), TOK_DEV)
    whole = pl.ds(pl.multiple_of(spots[0] * PAIR + at * TOK_DEV, TOK_DEV), TOK_DEV)
    for source, low, high in ((first_ref, 0, half), (second_ref, half, half + second_ref.shape[1])):

        def body(start):
            lanes = pl.ds(start - first, CBLK)
            total = source[whole, pl.ds(start - low, CBLK)] + rising_ref[local, lanes].astype(jnp.float32)
            total = total + falling_ref[local, lanes].astype(jnp.float32)
            out_ref[:, lanes] = total.astype(out_ref.dtype)

        if max(first, low) < min(stop, high):
            over_columns(max(first, low), min(stop, high), body)


def joined(spots, partials, bounds, rising, falling, swapped):
    kind = jnp.bfloat16 if swapped else jnp.float32
    return pl.pallas_call(
        functools.partial(join_kernel, bounds, swapped),
        in_specs=[SMEM_SPEC] + [VMEM_SPEC] * 4,
        out_specs=VMEM_SPEC,
        out_shape=pltpu.VMEM((TOK_DEV, bounds[1] - bounds[0]), kind),
        compiler_params=params(2),
        name="join",
    )(spots, *partials, in_vmem(rising), in_vmem(falling))


def sum_kernel(left_ref, right_ref, out_ref):
    out_ref[...] = left_ref[...] + right_ref[...]


def summed(left, right):
    return pl.pallas_call(
        sum_kernel,
        in_specs=[VMEM_SPEC] * 2,
        out_specs=VMEM_SPEC,
        out_shape=jax.ShapeDtypeStruct(left.shape, left.dtype),
        compiler_params=params(2),
        name="sum",
    )(left, right)


def finish_kernel(x_ref, gain_ref, mine0, other0, mine1, other1, left, right, out_ref, total_ref):
    total_ref[...] = left[...] + right[...]
    width = x_ref.shape[1]
    first = mine0.shape[1]
    squares = jnp.zeros((TOK_DEV, HEAD_DIM), jnp.float32)
    products = jnp.zeros((TOK_DEV, HEAD_DIM), jnp.float32)

    def at(start):
        mine, other, base = (mine0, other0, 0) if start < first else (mine1, other1, first)
        local = pl.ds(start - base, HEAD_DIM)
        grad = mine[:, local] + other[:, local].astype(jnp.float32)
        lanes = pl.ds(start, HEAD_DIM)
        return x_ref[:, lanes].astype(jnp.float32), gain_ref[:, lanes] * grad, lanes

    for start in range(0, width, HEAD_DIM):
        value, grad, _ = at(start)
        squares = squares + value * value
        products = products + grad * value
    scale = lax.rsqrt(jnp.sum(squares, axis=1, keepdims=True) / width + 1e-06)
    inner = scale * scale * scale * (jnp.sum(products, axis=1, keepdims=True) / width)
    for start in range(0, width, HEAD_DIM):
        value, grad, lanes = at(start)
        out_ref[:, lanes] = scale * grad - value * inner


def finished(tokens, gain, parts, sums):
    return pl.pallas_call(
        finish_kernel,
        out_shape=[
            jax.ShapeDtypeStruct(tokens.shape, jnp.float32),
            jax.ShapeDtypeStruct(gain.shape, jnp.float32),
        ],
        compiler_params=params(8),
        name="finish",
    )(tokens, gain, *parts, *sums)


def token_rows(spots, shift, swapped):
    side = 1 - spots[1] if swapped else spots[1]
    block = away(spots, shift) * (PAIR // TOK_DEV) + side
    return pl.ds(pl.multiple_of(block * TOK_DEV, TOK_DEV), TOK_DEV)


def norm_kernel(marks, spots, *refs):
    count = len(marks)
    xs, refs = refs[:count], refs[count:]
    first_ref, second_ref, gain_ref, refs = *refs[:3], refs[3:]
    normed_ref, total_ref = refs[-2:]
    width = gain_ref.shape[1]
    half = first_ref.shape[1]
    scales = []
    for j in range(count):

        def squares(at, total):
            for lane in range(0, CBLK, HEAD_DIM):
                lanes = pl.ds(pl.multiple_of(at * CBLK + lane, HEAD_DIM), HEAD_DIM)
                value = xs[j][:, lanes].astype(jnp.float32)
                total = total + value * value
            return total

        total = lax.fori_loop(0, width // CBLK, squares, jnp.zeros((TOK_DEV, HEAD_DIM), jnp.float32))
        scales.append(lax.rsqrt(jnp.sum(total, axis=1, keepdims=True) / width + 1e-06))

    for source, start in ((first_ref, 0), (second_ref, half)):

        def body(at):
            lanes = pl.ds(at, NBLK)
            gain = gain_ref[:, lanes]
            products = jnp.zeros((TOK_DEV, NBLK), jnp.float32)
            for j, mark in enumerate(marks):
                value = xs[j][:, lanes].astype(jnp.float32) * scales[j]
                products = products + source[token_rows(spots, *mark), pl.ds(at - start, NBLK)] * value
                normed_ref[j * TOK_DEV : (j + 1) * TOK_DEV, lanes] = (value * gain).astype(jnp.bfloat16)
            total = jnp.sum(products, axis=0, keepdims=True)
            if len(refs) > 2:
                total = total + refs[0][:, lanes]
            total_ref[:, lanes] = total

        over_columns(start, start + source.shape[1], body, NBLK)


def normalized(marks, spots, pieces, partials, gain, carried):
    count = len(pieces)
    width = gain.shape[1]
    return pl.pallas_call(
        functools.partial(norm_kernel, marks),
        in_specs=[SMEM_SPEC] + [VMEM_SPEC] * (count + 3 + len(carried)),
        out_specs=[VMEM_SPEC] * 2,
        out_shape=[
            pltpu.VMEM((count * TOK_DEV, width), jnp.bfloat16),
            pltpu.VMEM((1, width), jnp.float32),
        ],
        compiler_params=params(2),
        name="norm",
    )(spots, *[in_vmem(piece) for piece in pieces], *partials, gain, *carried)


def project_kernel(marks, spots, *refs):
    groups = len(marks)
    normed, refs = refs[:groups], refs[groups:]
    weight_ref, bias_ref, cos_ref, sin_ref = refs[:4]
    out_ref, acc_ref, stage_ref, out_sem = refs[-4:]
    acc_ref[...] = jnp.zeros_like(acc_ref)

    def body(at, block):
        lanes = pl.ds(pl.multiple_of(at * KBLK, KBLK), KBLK)
        values = [ref[:, lanes] for ref in normed]
        value = values[0] if groups == 1 else jnp.concatenate(values, axis=0)
        acc_ref[...] += jnp.dot(value, block, preferred_element_type=jnp.float32)

    over_weight(weight_ref, 0, weight_ref.shape[0] // KBLK, body)
    copies = []
    for j, mark in enumerate(mark for group in marks for mark in group):
        rows = pl.ds(j * TOK_DEV, TOK_DEV)
        whole = token_rows(spots, *mark)
        for head in range(stage_ref.shape[1] // HEAD_DIM):
            lanes = pl.ds(head * HEAD_DIM, HEAD_DIM)
            value = acc_ref[rows, lanes] + bias_ref[:, lanes]
            stage_ref[rows, lanes] = turn(
                value, cos_ref[whole, :], sin_ref[whole, :], spots[2 + head] == 1
            ).astype(jnp.bfloat16)
        copy = pltpu.make_async_copy(stage_ref.at[rows, :], out_ref.at[whole, :], out_sem.at[j])
        copy.start()
        copies.append(copy)
    for copy in copies:
        copy.wait()


def project(marks, spots, normed, weight, bias, cosine, sine, carried):
    rows, cols = sum(part.shape[0] for part in normed), weight.shape[1]
    in_specs = [SMEM_SPEC] + [VMEM_SPEC] * (len(normed) + 4)
    return pl.pallas_call(
        functools.partial(project_kernel, marks),
        in_specs=in_specs + [ANY_SPEC] * len(carried),
        out_specs=ANY_SPEC,
        out_shape=pltpu.HBM((cosine.shape[0], cols), jnp.bfloat16),
        scratch_shapes=[
            pltpu.VMEM((rows, cols), jnp.float32),
            pltpu.VMEM((rows, cols), jnp.bfloat16),
            pltpu.SemaphoreType.DMA((rows // TOK_DEV,)),
        ],
        input_output_aliases={len(in_specs): 0} if carried else {},
        compiler_params=params(4),
        name="project",
    )(spots, *normed, in_vmem(weight), bias, cosine, sine, *carried)


def work(tokens, norm_gain, qkv_weight, qkv_bias, qkv_grad):
    width, cols = qkv_weight.shape
    rows = qkv_grad.shape[0]
    heads = cols // HEAD_DIM
    ring = lax.axis_index("mp_0")
    side = lax.axis_index("mp_1")
    first_head = lax.axis_index(MP) * heads
    straight = ((first_head + jnp.arange(heads)) % GROUP == GROUP - 1).astype(jnp.int32)
    spots = jnp.concatenate([jnp.stack([ring, side]).astype(jnp.int32), straight])
    cosine, sine = tables(rows, SEQ_LEN // lax.axis_size(MP))
    bias_row = qkv_bias[None, :]
    spots, cosine, sine, gain_row, bias_row, qkv_grad = lax.optimization_barrier(
        (spots, cosine, sine, norm_gain[None, :], bias_row, qkv_grad)
    )
    cosine, sine, gain_row, bias_row = map(in_vmem, (cosine, sine, gain_row, bias_row))

    ups, downs = [tokens], [tokens]
    for _ in range(1, RING // 2 + 1):
        ups.append(up(ups[-1]))
    for _ in range(1, RING // 2):
        downs.append(down(downs[-1]))
    near = {"0": (0, tokens, swap(tokens))}
    for step in range(1, RING // 2 + 1):
        near[f"{step}u"] = (-step, ups[step], swap(ups[step]))
        if step < RING // 2:
            near[f"{step}d"] = (step, downs[step], swap(downs[step]))

    first, low, bias_grad = back_first(spots, qkv_grad, cosine, sine, qkv_weight)
    partials = (in_vmem(first), in_vmem(back_second(low, qkv_weight)))

    cut_a, cut_b, rest = (0, CUT), (CUT, width), (FIRST, width)
    far_u, far_d = (0, UP_FAR), (UP_FAR, FIRST)
    early = partials[:1] * 2

    def taken(at, span):
        return ((at, span),)

    rising, falling = added(spots, early, ((4, far_u, ()), (-4, far_d, ())), ())
    up4, down4a = up(rising), down(falling)
    (falling,) = added(spots, partials, ((-4, rest, ()),), ())
    down4b = down(falling)
    (rising,) = added(spots, partials, ((3, cut_a, taken(0, far_u)),), (up4,))
    up3a = up(rising)
    rising, falling = added(
        spots, partials, ((3, cut_b, ()), (-3, cut_a, taken(0, far_d) + taken(1, rest))), (down4a, down4b)
    )
    up3b, down3a = up(rising), down(falling)
    (falling,) = added(spots, partials, ((-3, cut_b, taken(0, rest)),), (down4b,))
    down3b = down(falling)
    rising, falling, later = added(
        spots,
        partials,
        ((2, cut_a, taken(0, cut_a)), (-2, cut_a, taken(1, cut_a)), (2, cut_b, taken(2, cut_b))),
        (up3a, down3a, up3b),
    )
    up2a, down2a, up2b = up(rising), down(falling), up(later)
    (falling,) = added(spots, partials, ((-2, cut_b, taken(0, cut_b)),), (down3b,))
    down2b = down(falling)
    parts = []
    for span, rising, falling in ((cut_a, up2a, down2a), (cut_b, up2b, down2b)):
        rising, falling = added(
            spots, partials, ((1, span, taken(0, span)), (-1, span, taken(1, span))), (rising, falling)
        )
        rising, falling = up(rising), down(falling)
        other = joined(spots, partials, span, rising, falling, True)
        mine = joined(spots, partials, span, rising, falling, False)
        parts += [mine, swap(other)]

    sums, batches = (), []
    for names in (("0", "1u"), ("1d", "2u"), ("2d", "3u"), ("3d", "4u")):
        group = [near[name] for name in names]
        pieces = [piece for _, piece, _ in group] + [piece for _, _, piece in group]
        marks = tuple((shift, swapped) for swapped in (False, True) for shift, _, _ in group)
        normed, total = normalized(marks, spots, pieces, partials, gain_row, sums)
        sums = (total,)
        batches.append((marks, normed))
    out = ()
    for batch in (batches[:1], batches[1:2], batches[2:3], batches[3:]):
        marks, normed = zip(*batch)
        out = (
            project(marks, spots, normed, qkv_weight, bias_row, cosine, sine, out),
        )

    total = summed(total, swap(total))
    for reach in (4, 1, 2):
        pairs = [(i, i ^ reach) for i in range(RING)]
        sums = (total, lax.ppermute(total, "mp_0", pairs))
        if reach != 2:
            total = summed(*sums)

    bias_grad, parts[2] = lax.optimization_barrier((bias_grad, parts[2]))
    tokens_grad, total = finished(tokens, gain_row, parts, sums)
    return (out[0], tokens_grad, total[0], bias_grad[0])


def solution(mesh):
    split = Mesh(mesh.devices.reshape(mesh.shape["dp"], 8, 2), ("dp", "mp_0", "mp_1"))
    placed = (P(DP_MP, None), P(), P(None, MP), P(MP), P("dp", MP))
    return jax.shard_map(
        work,
        mesh=split,
        in_specs=placed,
        out_specs=(P("dp", MP), P(DP_MP, None), P("dp"), P(DP_MP)),
        check_vma=False,
    )
```

```python
import functools

import jax
import jax.numpy as jnp
from jax import lax
from jax.experimental import pallas as pl
from jax.experimental.pallas import tpu as pltpu
from jax.sharding import Mesh
from jax.sharding import PartitionSpec as P

HEAD_DIM = 128
SEQ_LEN = 32768
GROUP = 10
TOK_DEV = 32
PAIR = 2 * TOK_DEV
RING = 8
MP = ("mp_0", "mp_1")
DP_MP = ("dp", "mp_0", "mp_1")
UP = [(i, (i + 1) % RING) for i in range(RING)]
DOWN = [(i, (i - 1) % RING) for i in range(RING)]
SWAP = [(0, 1), (1, 0)]
KBLK = 1024
FIRST = 3072
CBLK = 512
NBLK = 256
UP_FAR = 1024
UP_REST = 4096
CUT = 5120


def up(value):
    return lax.ppermute(value, "mp_0", UP)


def down(value):
    return lax.ppermute(value, "mp_0", DOWN)


def swap(value):
    return lax.ppermute(value, "mp_1", SWAP)


def tables(rows, stride):
    half = HEAD_DIM // 2
    row_index = jnp.arange(rows)
    place = row_index // TOK_DEV * stride + row_index % TOK_DEV
    inverse = jnp.exp(
        -jnp.log(jnp.float32(1000000.0)) * (2.0 * jnp.arange(half).astype(jnp.float32) / HEAD_DIM)
    )
    angle = place.astype(jnp.float32)[:, None] * inverse[None, :]
    cosine, sine = jnp.cos(angle), jnp.sin(angle)
    return (
        jnp.concatenate([cosine, cosine], axis=1),
        jnp.concatenate([-sine, sine], axis=1),
    )


def turn(value, cosine, sine, straight):
    cosine = jnp.where(straight, 1.0, cosine)
    sine = jnp.where(straight, 0.0, sine)
    return value * cosine + pltpu.roll(value, HEAD_DIM // 2, 1) * sine


def params(mib):
    return pltpu.CompilerParams(vmem_limit_bytes=mib << 20)


def in_vmem(value):
    return pltpu.with_memory_space_constraint(value, pltpu.VMEM)


VMEM_SPEC = pl.BlockSpec(memory_space=pltpu.VMEM)
SMEM_SPEC = pl.BlockSpec(memory_space=pltpu.SMEM)
ANY_SPEC = pl.BlockSpec(memory_space=pl.ANY)


def over_weight(weight_ref, first, count, body):
    def step(at, carry):
        body(at, weight_ref[pl.ds(pl.multiple_of((first + at) * KBLK, KBLK), KBLK), :])
        return carry

    lax.fori_loop(0, count, step, 0)


def over_copied(weight_ref, buffer_ref, sem, count, body):
    def copy(at):
        rows = pl.ds(pl.multiple_of(at * KBLK, KBLK), KBLK)
        return pltpu.make_async_copy(weight_ref.at[rows, :], buffer_ref.at[at % 2], sem.at[at % 2])

    copy(0).start()

    def step(at, carry):
        @pl.when(at + 1 < count)
        def _():
            copy(at + 1).start()

        copy(at).wait()
        body(at, buffer_ref[at % 2])
        return carry

    lax.fori_loop(0, count, step, 0)


def product(over, low_ref, out_ref):
    def body(at, block):
        lanes = pl.ds(pl.multiple_of(at * KBLK, KBLK), KBLK)
        out_ref[:, lanes] = lax.dot_general(
            low_ref[...], block, (((1,), (1,)), ((), ())), preferred_element_type=jnp.float32
        )

    over(out_ref.shape[1] // KBLK, body)


def rotate_kernel(spots, grad_ref, cos_ref, sin_ref, weight_ref, out_ref, low_ref, bias_ref, *scratch):
    for head in range(grad_ref.shape[1] // HEAD_DIM):
        lanes = pl.ds(head * HEAD_DIM, HEAD_DIM)
        value = grad_ref[:, lanes].astype(jnp.float32)
        turned = turn(value, cos_ref[...], -sin_ref[...], spots[2 + head] == 1)
        bias_ref[:, lanes] = jnp.sum(turned, axis=0, keepdims=True)
        low_ref[:, lanes] = turned.astype(jnp.bfloat16)
    product(functools.partial(over_copied, weight_ref, *scratch), low_ref, out_ref)


def back_first(spots, grad, cosine, sine, weight):
    rows, cols = grad.shape
    return pl.pallas_call(
        rotate_kernel,
        in_specs=[SMEM_SPEC] + [VMEM_SPEC] * 3 + [ANY_SPEC],
        out_specs=[VMEM_SPEC] * 3,
        out_shape=[
            pltpu.VMEM((rows, FIRST), jnp.float32),
            pltpu.VMEM((rows, cols), jnp.bfloat16),
            jax.ShapeDtypeStruct((1, cols), jnp.float32),
        ],
        scratch_shapes=[pltpu.VMEM((2, KBLK, cols), jnp.bfloat16), pltpu.SemaphoreType.DMA((2,))],
        compiler_params=params(6),
        name="back_first",
    )(spots, grad, cosine, sine, pltpu.with_memory_space_constraint(weight, pltpu.HBM))


def second_kernel(low_ref, weight_ref, out_ref):
    product(functools.partial(over_weight, weight_ref, FIRST // KBLK), low_ref, out_ref)


def back_second(low, weight):
    rows, _ = low.shape
    return pl.pallas_call(
        second_kernel,
        in_specs=[VMEM_SPEC] * 2,
        out_specs=VMEM_SPEC,
        out_shape=pltpu.VMEM((rows, weight.shape[0] - FIRST), jnp.float32),
        compiler_params=params(4),
        name="back_second",
    )(low, in_vmem(weight))


def over_columns(start, stop, body, block=CBLK):
    def step(at, carry):
        body(pl.multiple_of(start + at * block, block))
        return carry

    lax.fori_loop(0, (stop - start) // block, step, 0)


def away(spots, offset):
    return lax.rem(spots[0] + (offset + RING), RING)


def add_kernel(jobs, spots, first_ref, second_ref, *refs):
    half = first_ref.shape[1]
    arrived, outs = refs[: -len(jobs)], refs[-len(jobs) :]
    for (offset, (start, stop), taken), out_ref in zip(jobs, outs):
        rows = pl.ds(pl.multiple_of(away(spots, offset) * PAIR, PAIR), PAIR)
        spans = [span for _, span in taken]
        edges = {start, stop} | {e for span in ((half, half), *spans) for e in span if start < e < stop}
        edges = sorted(edges)
        for low, high in zip(edges[:-1], edges[1:]):
            source, base = (first_ref, 0) if low < half else (second_ref, half)
            adds = [(arrived[at], span[0]) for at, span in taken if span[0] <= low < span[1]]

            block = CBLK if (high - low) % CBLK == 0 else CBLK // 2

            def body(at):
                total = source[rows, pl.ds(at - base, block)]
                for ref, begin in adds:
                    total = total + ref[:, pl.ds(at - begin, block)].astype(jnp.float32)
                out_ref[:, pl.ds(at - start, block)] = total.astype(jnp.bfloat16)

            over_columns(low, high, body, block)


def added(spots, partials, jobs, arrived):
    return pl.pallas_call(
        functools.partial(add_kernel, jobs),
        in_specs=[SMEM_SPEC] + [VMEM_SPEC] * (2 + len(arrived)),
        out_specs=[VMEM_SPEC] * len(jobs),
        out_shape=[pltpu.VMEM((PAIR, stop - start), jnp.bfloat16) for _, (start, stop), _ in jobs],
        compiler_params=params(2),
        name="add",
    )(spots, *partials, *[in_vmem(value) for value in arrived])


def join_kernel(bounds, spots, first_ref, second_ref, rising_ref, falling_ref, mine_ref, other_ref):
    first, stop = bounds
    half = first_ref.shape[1]
    for at, out_ref in ((spots[1], mine_ref), (1 - spots[1], other_ref)):
        local = pl.ds(pl.multiple_of(at * TOK_DEV, TOK_DEV), TOK_DEV)
        whole = pl.ds(pl.multiple_of(spots[0] * PAIR + at * TOK_DEV, TOK_DEV), TOK_DEV)
        for source, low, high in ((first_ref, 0, half), (second_ref, half, half + second_ref.shape[1])):

            def body(start):
                lanes = pl.ds(start - first, CBLK)
                total = source[whole, pl.ds(start - low, CBLK)] + rising_ref[local, lanes].astype(jnp.float32)
                total = total + falling_ref[local, lanes].astype(jnp.float32)
                out_ref[:, lanes] = total.astype(out_ref.dtype)

            if max(first, low) < min(stop, high):
                over_columns(max(first, low), min(stop, high), body)


def joined(spots, partials, bounds, rising, falling):
    span = bounds[1] - bounds[0]
    return pl.pallas_call(
        functools.partial(join_kernel, bounds),
        in_specs=[SMEM_SPEC] + [VMEM_SPEC] * 4,
        out_specs=[VMEM_SPEC] * 2,
        out_shape=[
            pltpu.VMEM((TOK_DEV, span), jnp.float32),
            pltpu.VMEM((TOK_DEV, span), jnp.bfloat16),
        ],
        compiler_params=params(2),
        name="join",
    )(spots, *partials, in_vmem(rising), in_vmem(falling))


def sum_kernel(left_ref, right_ref, out_ref):
    out_ref[...] = left_ref[...] + right_ref[...]


def summed(left, right):
    return pl.pallas_call(
        sum_kernel,
        in_specs=[VMEM_SPEC] * 2,
        out_specs=VMEM_SPEC,
        out_shape=jax.ShapeDtypeStruct(left.shape, left.dtype),
        compiler_params=params(2),
        name="sum",
    )(left, right)


def finish_kernel(x_ref, gain_ref, mine0, other0, mine1, other1, left, right, out_ref, total_ref):
    total_ref[...] = left[...] + right[...]
    width = x_ref.shape[1]
    first = mine0.shape[1]
    squares = jnp.zeros((TOK_DEV, HEAD_DIM), jnp.float32)
    products = jnp.zeros((TOK_DEV, HEAD_DIM), jnp.float32)

    def at(start):
        mine, other, base = (mine0, other0, 0) if start < first else (mine1, other1, first)
        local = pl.ds(start - base, HEAD_DIM)
        grad = mine[:, local] + other[:, local].astype(jnp.float32)
        lanes = pl.ds(start, HEAD_DIM)
        return x_ref[:, lanes].astype(jnp.float32), gain_ref[:, lanes] * grad, lanes

    for start in range(0, width, HEAD_DIM):
        value, grad, _ = at(start)
        squares = squares + value * value
        products = products + grad * value
    scale = lax.rsqrt(jnp.sum(squares, axis=1, keepdims=True) / width + 1e-06)
    inner = scale * scale * scale * (jnp.sum(products, axis=1, keepdims=True) / width)
    for start in range(0, width, HEAD_DIM):
        value, grad, lanes = at(start)
        out_ref[:, lanes] = scale * grad - value * inner


def finished(tokens, gain, parts, sums):
    return pl.pallas_call(
        finish_kernel,
        out_shape=[
            jax.ShapeDtypeStruct(tokens.shape, jnp.float32),
            jax.ShapeDtypeStruct(gain.shape, jnp.float32),
        ],
        compiler_params=params(8),
        name="finish",
    )(tokens, gain, *parts, *sums)


def token_rows(spots, shift, swapped):
    side = 1 - spots[1] if swapped else spots[1]
    block = away(spots, shift) * (PAIR // TOK_DEV) + side
    return pl.ds(pl.multiple_of(block * TOK_DEV, TOK_DEV), TOK_DEV)


def norm_kernel(marks, spots, *refs):
    count = len(marks)
    xs, refs = refs[:count], refs[count:]
    first_ref, second_ref, gain_ref, refs = *refs[:3], refs[3:]
    normed_ref, total_ref = refs[-2:]
    width = gain_ref.shape[1]
    half = first_ref.shape[1]
    scales = []
    for j in range(count):

        def squares(at, total):
            for lane in range(0, CBLK, HEAD_DIM):
                lanes = pl.ds(pl.multiple_of(at * CBLK + lane, HEAD_DIM), HEAD_DIM)
                value = xs[j][:, lanes].astype(jnp.float32)
                total = total + value * value
            return total

        total = lax.fori_loop(0, width // CBLK, squares, jnp.zeros((TOK_DEV, HEAD_DIM), jnp.float32))
        scales.append(lax.rsqrt(jnp.sum(total, axis=1, keepdims=True) / width + 1e-06))

    for source, start in ((first_ref, 0), (second_ref, half)):

        def body(at):
            lanes = pl.ds(at, NBLK)
            gain = gain_ref[:, lanes]
            products = jnp.zeros((TOK_DEV, NBLK), jnp.float32)
            for j, mark in enumerate(marks):
                value = xs[j][:, lanes].astype(jnp.float32) * scales[j]
                products = products + source[token_rows(spots, *mark), pl.ds(at - start, NBLK)] * value
                normed_ref[j * TOK_DEV : (j + 1) * TOK_DEV, lanes] = (value * gain).astype(jnp.bfloat16)
            total = jnp.sum(products, axis=0, keepdims=True)
            if len(refs) > 2:
                total = total + refs[0][:, lanes]
            total_ref[:, lanes] = total

        over_columns(start, start + source.shape[1], body, NBLK)


def normalized(marks, spots, pieces, partials, gain, carried):
    count = len(pieces)
    width = gain.shape[1]
    return pl.pallas_call(
        functools.partial(norm_kernel, marks),
        in_specs=[SMEM_SPEC] + [VMEM_SPEC] * (count + 3 + len(carried)),
        out_specs=[VMEM_SPEC] * 2,
        out_shape=[
            pltpu.VMEM((count * TOK_DEV, width), jnp.bfloat16),
            pltpu.VMEM((1, width), jnp.float32),
        ],
        compiler_params=params(2),
        name="norm",
    )(spots, *[in_vmem(piece) for piece in pieces], *partials, gain, *carried)


def project_kernel(marks, spots, *refs):
    groups = len(marks)
    normed, refs = refs[:groups], refs[groups:]
    weight_ref, bias_ref, cos_ref, sin_ref = refs[:4]
    out_ref, acc_ref, stage_ref, out_sem = refs[-4:]
    acc_ref[...] = jnp.zeros_like(acc_ref)

    def body(at, block):
        lanes = pl.ds(pl.multiple_of(at * KBLK, KBLK), KBLK)
        values = [ref[:, lanes] for ref in normed]
        value = values[0] if groups == 1 else jnp.concatenate(values, axis=0)
        acc_ref[...] += jnp.dot(value, block, preferred_element_type=jnp.float32)

    over_weight(weight_ref, 0, weight_ref.shape[0] // KBLK, body)
    copies = []
    for j, mark in enumerate(mark for group in marks for mark in group):
        rows = pl.ds(j * TOK_DEV, TOK_DEV)
        whole = token_rows(spots, *mark)
        for head in range(stage_ref.shape[1] // HEAD_DIM):
            lanes = pl.ds(head * HEAD_DIM, HEAD_DIM)
            value = acc_ref[rows, lanes] + bias_ref[:, lanes]
            stage_ref[rows, lanes] = turn(
                value, cos_ref[whole, :], sin_ref[whole, :], spots[2 + head] == 1
            ).astype(jnp.bfloat16)
        copy = pltpu.make_async_copy(stage_ref.at[rows, :], out_ref.at[whole, :], out_sem.at[j])
        copy.start()
        copies.append(copy)
    for copy in copies:
        copy.wait()


def project(marks, spots, normed, weight, bias, cosine, sine, carried):
    rows, cols = sum(part.shape[0] for part in normed), weight.shape[1]
    in_specs = [SMEM_SPEC] + [VMEM_SPEC] * (len(normed) + 4)
    return pl.pallas_call(
        functools.partial(project_kernel, marks),
        in_specs=in_specs + [ANY_SPEC] * len(carried),
        out_specs=ANY_SPEC,
        out_shape=pltpu.HBM((cosine.shape[0], cols), jnp.bfloat16),
        scratch_shapes=[
            pltpu.VMEM((rows, cols), jnp.float32),
            pltpu.VMEM((rows, cols), jnp.bfloat16),
            pltpu.SemaphoreType.DMA((rows // TOK_DEV,)),
        ],
        input_output_aliases={len(in_specs): 0} if carried else {},
        compiler_params=params(4),
        name="project",
    )(spots, *normed, in_vmem(weight), bias, cosine, sine, *carried)


def work(tokens, norm_gain, qkv_weight, qkv_bias, qkv_grad):
    width, cols = qkv_weight.shape
    rows = qkv_grad.shape[0]
    heads = cols // HEAD_DIM
    ring = lax.axis_index("mp_0")
    side = lax.axis_index("mp_1")
    first_head = lax.axis_index(MP) * heads
    straight = ((first_head + jnp.arange(heads)) % GROUP == GROUP - 1).astype(jnp.int32)
    spots = jnp.concatenate([jnp.stack([ring, side]).astype(jnp.int32), straight])
    cosine, sine = tables(rows, SEQ_LEN // lax.axis_size(MP))
    bias_row = qkv_bias[None, :]
    spots, cosine, sine, gain_row, bias_row, qkv_grad = lax.optimization_barrier(
        (spots, cosine, sine, norm_gain[None, :], bias_row, qkv_grad)
    )
    cosine, sine, gain_row, bias_row = map(in_vmem, (cosine, sine, gain_row, bias_row))

    ups, downs = [tokens], [tokens]
    for _ in range(1, RING // 2 + 1):
        ups.append(up(ups[-1]))
    for _ in range(1, RING // 2):
        downs.append(down(downs[-1]))
    near = {"0": (0, tokens, swap(tokens))}
    for step in range(1, RING // 2 + 1):
        near[f"{step}u"] = (-step, ups[step], swap(ups[step]))
        if step < RING // 2:
            near[f"{step}d"] = (step, downs[step], swap(downs[step]))

    first, low, bias_grad = back_first(spots, qkv_grad, cosine, sine, qkv_weight)
    partials = (in_vmem(first), in_vmem(back_second(low, qkv_weight)))

    cut_a, cut_b = (0, CUT), (CUT, width)
    far_u, far_d = (0, UP_FAR), (UP_FAR, FIRST)
    rest_u, rest_d = (FIRST, UP_REST), (UP_REST, width)
    early = partials[:1] * 2

    def taken(at, span):
        return ((at, span),)

    rising, falling = added(spots, early, ((4, far_u, ()), (-4, far_d, ())), ())
    up4, down4a = up(rising), down(falling)
    later, rising, falling = added(spots, partials, ((3, cut_b, ()), (4, rest_u, ()), (-4, rest_d, ())), ())
    up3b, up4b, down4b = up(later), up(rising), down(falling)
    rising, falling = added(
        spots,
        partials,
        ((3, cut_a, taken(0, far_u) + taken(1, rest_u)), (-3, cut_a, taken(2, far_d) + taken(3, rest_d))),
        (up4, up4b, down4a, down4b),
    )
    up3a, down3a = up(rising), down(falling)
    (falling,) = added(spots, partials, ((-3, cut_b, taken(0, rest_d)),), (down4b,))
    down3b = down(falling)
    rising, falling, later = added(
        spots,
        partials,
        ((2, cut_a, taken(0, cut_a)), (-2, cut_a, taken(1, cut_a)), (2, cut_b, taken(2, cut_b))),
        (up3a, down3a, up3b),
    )
    up2a, down2a, up2b = up(rising), down(falling), up(later)
    (falling,) = added(spots, partials, ((-2, cut_b, taken(0, cut_b)),), (down3b,))
    down2b = down(falling)
    parts = []
    for span, rising, falling in ((cut_a, up2a, down2a), (cut_b, up2b, down2b)):
        rising, falling = added(
            spots, partials, ((1, span, taken(0, span)), (-1, span, taken(1, span))), (rising, falling)
        )
        rising, falling = up(rising), down(falling)
        mine, other = joined(spots, partials, span, rising, falling)
        parts += [mine, swap(other)]

    sums, batches = (), []
    for names in (("0", "1u"), ("1d", "2u"), ("2d", "3u"), ("3d", "4u")):
        group = [near[name] for name in names]
        pieces = [piece for _, piece, _ in group] + [piece for _, _, piece in group]
        marks = tuple((shift, swapped) for swapped in (False, True) for shift, _, _ in group)
        normed, total = normalized(marks, spots, pieces, partials, gain_row, sums)
        sums = (total,)
        batches.append((marks, normed))
    out = ()
    for batch in (batches[:1], batches[1:2], batches[2:3], batches[3:]):
        marks, normed = zip(*batch)
        out = (
            project(marks, spots, normed, qkv_weight, bias_row, cosine, sine, out),
        )

    total = summed(total, swap(total))
    for reach in (4, 1, 2):
        pairs = [(i, i ^ reach) for i in range(RING)]
        sums = (total, lax.ppermute(total, "mp_0", pairs))
        if reach != 2:
            total = summed(*sums)

    bias_grad, parts[2] = lax.optimization_barrier((bias_grad, parts[2]))
    tokens_grad, total = finished(tokens, gain_row, parts, sums)
    return (out[0], tokens_grad, total[0], bias_grad[0])


def solution(mesh):
    split = Mesh(mesh.devices.reshape(mesh.shape["dp"], 8, 2), ("dp", "mp_0", "mp_1"))
    placed = (P(DP_MP, None), P(), P(None, MP), P(MP), P("dp", MP))
    return jax.shard_map(
        work,
        mesh=split,
        in_specs=placed,
        out_specs=(P("dp", MP), P(DP_MP, None), P("dp"), P(DP_MP)),
        check_vma=False,
    )
```

```python
import functools

import jax
import jax.numpy as jnp
from jax import lax
from jax.experimental import pallas as pl
from jax.experimental.pallas import tpu as pltpu
from jax.sharding import Mesh
from jax.sharding import PartitionSpec as P

HEAD_DIM = 128
SEQ_LEN = 32768
GROUP = 10
TOK_DEV = 32
PAIR = 2 * TOK_DEV
RING = 8
MP = ("mp_0", "mp_1")
DP_MP = ("dp", "mp_0", "mp_1")
UP = [(i, (i + 1) % RING) for i in range(RING)]
DOWN = [(i, (i - 1) % RING) for i in range(RING)]
SWAP = [(0, 1), (1, 0)]
KBLK = 1024
FIRST = 3072
CBLK = 512
NBLK = 256
UP_FAR = 1024
UP_REST = 4096
CUT = 5120


def up(value):
    return lax.ppermute(value, "mp_0", UP)


def down(value):
    return lax.ppermute(value, "mp_0", DOWN)


def swap(value):
    return lax.ppermute(value, "mp_1", SWAP)


def tables(rows, stride):
    half = HEAD_DIM // 2
    row_index = jnp.arange(rows)
    place = row_index // TOK_DEV * stride + row_index % TOK_DEV
    inverse = jnp.exp(
        -jnp.log(jnp.float32(1000000.0)) * (2.0 * jnp.arange(half).astype(jnp.float32) / HEAD_DIM)
    )
    angle = place.astype(jnp.float32)[:, None] * inverse[None, :]
    cosine, sine = jnp.cos(angle), jnp.sin(angle)
    return (
        jnp.concatenate([cosine, cosine], axis=1),
        jnp.concatenate([-sine, sine], axis=1),
    )


def turn(value, cosine, sine, straight):
    cosine = jnp.where(straight, 1.0, cosine)
    sine = jnp.where(straight, 0.0, sine)
    return value * cosine + pltpu.roll(value, HEAD_DIM // 2, 1) * sine


def params(mib):
    return pltpu.CompilerParams(vmem_limit_bytes=mib << 20)


def in_vmem(value):
    return pltpu.with_memory_space_constraint(value, pltpu.VMEM)


VMEM_SPEC = pl.BlockSpec(memory_space=pltpu.VMEM)
SMEM_SPEC = pl.BlockSpec(memory_space=pltpu.SMEM)
ANY_SPEC = pl.BlockSpec(memory_space=pl.ANY)


def over_weight(weight_ref, first, count, body):
    def step(at, carry):
        body(at, weight_ref[pl.ds(pl.multiple_of((first + at) * KBLK, KBLK), KBLK), :])
        return carry

    lax.fori_loop(0, count, step, 0)


def over_copied(weight_ref, buffer_ref, sem, count, body):
    def copy(at):
        rows = pl.ds(pl.multiple_of(at * KBLK, KBLK), KBLK)
        return pltpu.make_async_copy(weight_ref.at[rows, :], buffer_ref.at[at % 2], sem.at[at % 2])

    copy(0).start()

    def step(at, carry):
        @pl.when(at + 1 < count)
        def _():
            copy(at + 1).start()

        copy(at).wait()
        body(at, buffer_ref[at % 2])
        return carry

    lax.fori_loop(0, count, step, 0)


def product(over, low_ref, out_ref):
    def body(at, block):
        lanes = pl.ds(pl.multiple_of(at * KBLK, KBLK), KBLK)
        out_ref[:, lanes] = lax.dot_general(
            low_ref[...], block, (((1,), (1,)), ((), ())), preferred_element_type=jnp.float32
        )

    over(out_ref.shape[1] // KBLK, body)


def rotate_kernel(spots, grad_ref, cos_ref, sin_ref, weight_ref, out_ref, low_ref, bias_ref, *scratch):
    for head in range(grad_ref.shape[1] // HEAD_DIM):
        lanes = pl.ds(head * HEAD_DIM, HEAD_DIM)
        value = grad_ref[:, lanes].astype(jnp.float32)
        turned = turn(value, cos_ref[...], -sin_ref[...], spots[2 + head] == 1)
        bias_ref[:, lanes] = jnp.sum(turned, axis=0, keepdims=True)
        low_ref[:, lanes] = turned.astype(jnp.bfloat16)
    product(functools.partial(over_copied, weight_ref, *scratch), low_ref, out_ref)


def back_first(spots, grad, cosine, sine, weight):
    rows, cols = grad.shape
    return pl.pallas_call(
        rotate_kernel,
        in_specs=[SMEM_SPEC] + [VMEM_SPEC] * 3 + [ANY_SPEC],
        out_specs=[VMEM_SPEC] * 3,
        out_shape=[
            pltpu.VMEM((rows, FIRST), jnp.float32),
            pltpu.VMEM((rows, cols), jnp.bfloat16),
            jax.ShapeDtypeStruct((1, cols), jnp.float32),
        ],
        scratch_shapes=[pltpu.VMEM((2, KBLK, cols), jnp.bfloat16), pltpu.SemaphoreType.DMA((2,))],
        compiler_params=params(6),
        name="back_first",
    )(spots, grad, cosine, sine, pltpu.with_memory_space_constraint(weight, pltpu.HBM))


def second_kernel(low_ref, weight_ref, out_ref):
    product(functools.partial(over_weight, weight_ref, FIRST // KBLK), low_ref, out_ref)


def back_second(low, weight):
    rows, _ = low.shape
    return pl.pallas_call(
        second_kernel,
        in_specs=[VMEM_SPEC] * 2,
        out_specs=VMEM_SPEC,
        out_shape=pltpu.VMEM((rows, weight.shape[0] - FIRST), jnp.float32),
        compiler_params=params(4),
        name="back_second",
    )(low, in_vmem(weight))


def over_columns(start, stop, body, block=CBLK):
    def step(at, carry):
        body(pl.multiple_of(start + at * block, block))
        return carry

    lax.fori_loop(0, (stop - start) // block, step, 0)


def away(spots, offset):
    return lax.rem(spots[0] + (offset + RING), RING)


def add_kernel(jobs, spots, first_ref, second_ref, *refs):
    half = first_ref.shape[1]
    arrived, outs = refs[: -len(jobs)], refs[-len(jobs) :]
    for (offset, (start, stop), taken), out_ref in zip(jobs, outs):
        rows = pl.ds(pl.multiple_of(away(spots, offset) * PAIR, PAIR), PAIR)
        spans = [span for _, span in taken]
        edges = {start, stop} | {e for span in ((half, half), *spans) for e in span if start < e < stop}
        edges = sorted(edges)
        for low, high in zip(edges[:-1], edges[1:]):
            source, base = (first_ref, 0) if low < half else (second_ref, half)
            adds = [(arrived[at], span[0]) for at, span in taken if span[0] <= low < span[1]]

            block = CBLK if (high - low) % CBLK == 0 else CBLK // 2

            def body(at):
                total = source[rows, pl.ds(at - base, block)]
                for ref, begin in adds:
                    total = total + ref[:, pl.ds(at - begin, block)].astype(jnp.float32)
                out_ref[:, pl.ds(at - start, block)] = total.astype(jnp.bfloat16)

            over_columns(low, high, body, block)


def added(spots, partials, jobs, arrived):
    return pl.pallas_call(
        functools.partial(add_kernel, jobs),
        in_specs=[SMEM_SPEC] + [VMEM_SPEC] * (2 + len(arrived)),
        out_specs=[VMEM_SPEC] * len(jobs),
        out_shape=[pltpu.VMEM((PAIR, stop - start), jnp.bfloat16) for _, (start, stop), _ in jobs],
        compiler_params=params(2),
        name="add",
    )(spots, *partials, *[in_vmem(value) for value in arrived])


def join_kernel(bounds, spots, first_ref, second_ref, rising_ref, falling_ref, mine_ref, other_ref):
    first, stop = bounds
    half = first_ref.shape[1]
    for at, out_ref in ((spots[1], mine_ref), (1 - spots[1], other_ref)):
        local = pl.ds(pl.multiple_of(at * TOK_DEV, TOK_DEV), TOK_DEV)
        whole = pl.ds(pl.multiple_of(spots[0] * PAIR + at * TOK_DEV, TOK_DEV), TOK_DEV)
        for source, low, high in ((first_ref, 0, half), (second_ref, half, half + second_ref.shape[1])):

            def body(start):
                lanes = pl.ds(start - first, CBLK)
                total = source[whole, pl.ds(start - low, CBLK)] + rising_ref[local, lanes].astype(jnp.float32)
                total = total + falling_ref[local, lanes].astype(jnp.float32)
                out_ref[:, lanes] = total.astype(out_ref.dtype)

            if max(first, low) < min(stop, high):
                over_columns(max(first, low), min(stop, high), body)


def joined(spots, partials, bounds, rising, falling):
    span = bounds[1] - bounds[0]
    return pl.pallas_call(
        functools.partial(join_kernel, bounds),
        in_specs=[SMEM_SPEC] + [VMEM_SPEC] * 4,
        out_specs=[VMEM_SPEC] * 2,
        out_shape=[
            pltpu.VMEM((TOK_DEV, span), jnp.float32),
            pltpu.VMEM((TOK_DEV, span), jnp.bfloat16),
        ],
        compiler_params=params(2),
        name="join",
    )(spots, *partials, in_vmem(rising), in_vmem(falling))


def sum_kernel(left_ref, right_ref, out_ref):
    out_ref[...] = left_ref[...] + right_ref[...]


def summed(left, right):
    return pl.pallas_call(
        sum_kernel,
        in_specs=[VMEM_SPEC] * 2,
        out_specs=VMEM_SPEC,
        out_shape=jax.ShapeDtypeStruct(left.shape, left.dtype),
        compiler_params=params(2),
        name="sum",
    )(left, right)


def finish_kernel(x_ref, gain_ref, mine0, other0, mine1, other1, own, one, two, three, out_ref, total_ref):
    total_ref[...] = (own[...] + one[...]) + (two[...] + three[...])
    width = x_ref.shape[1]
    first = mine0.shape[1]
    squares = jnp.zeros((TOK_DEV, HEAD_DIM), jnp.float32)
    products = jnp.zeros((TOK_DEV, HEAD_DIM), jnp.float32)

    def at(start):
        mine, other, base = (mine0, other0, 0) if start < first else (mine1, other1, first)
        local = pl.ds(start - base, HEAD_DIM)
        grad = mine[:, local] + other[:, local].astype(jnp.float32)
        lanes = pl.ds(start, HEAD_DIM)
        return x_ref[:, lanes].astype(jnp.float32), gain_ref[:, lanes] * grad, lanes

    for start in range(0, width, HEAD_DIM):
        value, grad, _ = at(start)
        squares = squares + value * value
        products = products + grad * value
    scale = lax.rsqrt(jnp.sum(squares, axis=1, keepdims=True) / width + 1e-06)
    inner = scale * scale * scale * (jnp.sum(products, axis=1, keepdims=True) / width)
    for start in range(0, width, HEAD_DIM):
        value, grad, lanes = at(start)
        out_ref[:, lanes] = scale * grad - value * inner


def finished(tokens, gain, parts, sums):
    return pl.pallas_call(
        finish_kernel,
        out_shape=[
            jax.ShapeDtypeStruct(tokens.shape, jnp.float32),
            jax.ShapeDtypeStruct(gain.shape, jnp.float32),
        ],
        compiler_params=params(8),
        name="finish",
    )(tokens, gain, *parts, *sums)


def token_rows(spots, shift, swapped):
    side = 1 - spots[1] if swapped else spots[1]
    block = away(spots, shift) * (PAIR // TOK_DEV) + side
    return pl.ds(pl.multiple_of(block * TOK_DEV, TOK_DEV), TOK_DEV)


def norm_kernel(marks, spots, *refs):
    count = len(marks)
    xs, refs = refs[:count], refs[count:]
    first_ref, second_ref, gain_ref, refs = *refs[:3], refs[3:]
    normed_ref, total_ref = refs[-2:]
    width = gain_ref.shape[1]
    half = first_ref.shape[1]
    scales = []
    for j in range(count):

        def squares(at, total):
            for lane in range(0, CBLK, HEAD_DIM):
                lanes = pl.ds(pl.multiple_of(at * CBLK + lane, HEAD_DIM), HEAD_DIM)
                value = xs[j][:, lanes].astype(jnp.float32)
                total = total + value * value
            return total

        total = lax.fori_loop(0, width // CBLK, squares, jnp.zeros((TOK_DEV, HEAD_DIM), jnp.float32))
        scales.append(lax.rsqrt(jnp.sum(total, axis=1, keepdims=True) / width + 1e-06))

    for source, start in ((first_ref, 0), (second_ref, half)):

        def body(at):
            lanes = pl.ds(at, NBLK)
            gain = gain_ref[:, lanes]
            products = jnp.zeros((TOK_DEV, NBLK), jnp.float32)
            for j, mark in enumerate(marks):
                value = xs[j][:, lanes].astype(jnp.float32) * scales[j]
                products = products + source[token_rows(spots, *mark), pl.ds(at - start, NBLK)] * value
                normed_ref[j * TOK_DEV : (j + 1) * TOK_DEV, lanes] = (value * gain).astype(jnp.bfloat16)
            total = jnp.sum(products, axis=0, keepdims=True)
            if len(refs) > 2:
                total = total + refs[0][:, lanes]
            total_ref[:, lanes] = total

        over_columns(start, start + source.shape[1], body, NBLK)


def normalized(marks, spots, pieces, partials, gain, carried):
    count = len(pieces)
    width = gain.shape[1]
    return pl.pallas_call(
        functools.partial(norm_kernel, marks),
        in_specs=[SMEM_SPEC] + [VMEM_SPEC] * (count + 3 + len(carried)),
        out_specs=[VMEM_SPEC] * 2,
        out_shape=[
            pltpu.VMEM((count * TOK_DEV, width), jnp.bfloat16),
            pltpu.VMEM((1, width), jnp.float32),
        ],
        compiler_params=params(2),
        name="norm",
    )(spots, *[in_vmem(piece) for piece in pieces], *partials, gain, *carried)


def project_kernel(marks, spots, *refs):
    groups = len(marks)
    normed, refs = refs[:groups], refs[groups:]
    weight_ref, bias_ref, cos_ref, sin_ref = refs[:4]
    out_ref, acc_ref, stage_ref, out_sem = refs[-4:]
    acc_ref[...] = jnp.zeros_like(acc_ref)

    def body(at, block):
        lanes = pl.ds(pl.multiple_of(at * KBLK, KBLK), KBLK)
        values = [ref[:, lanes] for ref in normed]
        value = values[0] if groups == 1 else jnp.concatenate(values, axis=0)
        acc_ref[...] += jnp.dot(value, block, preferred_element_type=jnp.float32)

    over_weight(weight_ref, 0, weight_ref.shape[0] // KBLK, body)
    copies = []
    for j, mark in enumerate(mark for group in marks for mark in group):
        rows = pl.ds(j * TOK_DEV, TOK_DEV)
        whole = token_rows(spots, *mark)
        for head in range(stage_ref.shape[1] // HEAD_DIM):
            lanes = pl.ds(head * HEAD_DIM, HEAD_DIM)
            value = acc_ref[rows, lanes] + bias_ref[:, lanes]
            stage_ref[rows, lanes] = turn(
                value, cos_ref[whole, :], sin_ref[whole, :], spots[2 + head] == 1
            ).astype(jnp.bfloat16)
        copy = pltpu.make_async_copy(stage_ref.at[rows, :], out_ref.at[whole, :], out_sem.at[j])
        copy.start()
        copies.append(copy)
    for copy in copies:
        copy.wait()


def project(marks, spots, normed, weight, bias, cosine, sine, carried):
    rows, cols = sum(part.shape[0] for part in normed), weight.shape[1]
    in_specs = [SMEM_SPEC] + [VMEM_SPEC] * (len(normed) + 4)
    return pl.pallas_call(
        functools.partial(project_kernel, marks),
        in_specs=in_specs + [ANY_SPEC] * len(carried),
        out_specs=ANY_SPEC,
        out_shape=pltpu.HBM((cosine.shape[0], cols), jnp.bfloat16),
        scratch_shapes=[
            pltpu.VMEM((rows, cols), jnp.float32),
            pltpu.VMEM((rows, cols), jnp.bfloat16),
            pltpu.SemaphoreType.DMA((rows // TOK_DEV,)),
        ],
        input_output_aliases={len(in_specs): 0} if carried else {},
        compiler_params=params(4),
        name="project",
    )(spots, *normed, in_vmem(weight), bias, cosine, sine, *carried)


def work(tokens, norm_gain, qkv_weight, qkv_bias, qkv_grad):
    width, cols = qkv_weight.shape
    rows = qkv_grad.shape[0]
    heads = cols // HEAD_DIM
    ring = lax.axis_index("mp_0")
    side = lax.axis_index("mp_1")
    first_head = lax.axis_index(MP) * heads
    straight = ((first_head + jnp.arange(heads)) % GROUP == GROUP - 1).astype(jnp.int32)
    spots = jnp.concatenate([jnp.stack([ring, side]).astype(jnp.int32), straight])
    cosine, sine = tables(rows, SEQ_LEN // lax.axis_size(MP))
    bias_row = qkv_bias[None, :]
    spots, cosine, sine, gain_row, bias_row, qkv_grad = lax.optimization_barrier(
        (spots, cosine, sine, norm_gain[None, :], bias_row, qkv_grad)
    )
    cosine, sine, gain_row, bias_row = map(in_vmem, (cosine, sine, gain_row, bias_row))

    ups, downs = [tokens], [tokens]
    for _ in range(1, RING // 2 + 1):
        ups.append(up(ups[-1]))
    for _ in range(1, RING // 2):
        downs.append(down(downs[-1]))
    near = {"0": (0, tokens, swap(tokens))}
    for step in range(1, RING // 2 + 1):
        near[f"{step}u"] = (-step, ups[step], swap(ups[step]))
        if step < RING // 2:
            near[f"{step}d"] = (step, downs[step], swap(downs[step]))

    first, low, bias_grad = back_first(spots, qkv_grad, cosine, sine, qkv_weight)
    partials = (in_vmem(first), in_vmem(back_second(low, qkv_weight)))

    cut_a, cut_b = (0, CUT), (CUT, width)
    far_u, far_d = (0, UP_FAR), (UP_FAR, FIRST)
    rest_u, rest_d = (FIRST, UP_REST), (UP_REST, width)
    early = partials[:1] * 2

    def taken(at, span):
        return ((at, span),)

    rising, falling = added(spots, early, ((4, far_u, ()), (-4, far_d, ())), ())
    up4, down4a = up(rising), down(falling)
    later, rising, falling = added(spots, partials, ((3, cut_b, ()), (4, rest_u, ()), (-4, rest_d, ())), ())
    up3b, up4b, down4b = up(later), up(rising), down(falling)
    rising, falling = added(
        spots,
        partials,
        ((3, cut_a, taken(0, far_u) + taken(1, rest_u)), (-3, cut_a, taken(2, far_d) + taken(3, rest_d))),
        (up4, up4b, down4a, down4b),
    )
    up3a, down3a = up(rising), down(falling)
    (falling,) = added(spots, partials, ((-3, cut_b, taken(0, rest_d)),), (down4b,))
    down3b = down(falling)
    rising, falling, later = added(
        spots,
        partials,
        ((2, cut_a, taken(0, cut_a)), (-2, cut_a, taken(1, cut_a)), (2, cut_b, taken(2, cut_b))),
        (up3a, down3a, up3b),
    )
    up2a, down2a, up2b = up(rising), down(falling), up(later)
    (falling,) = added(spots, partials, ((-2, cut_b, taken(0, cut_b)),), (down3b,))
    down2b = down(falling)
    parts = []
    for span, rising, falling in ((cut_a, up2a, down2a), (cut_b, up2b, down2b)):
        rising, falling = added(
            spots, partials, ((1, span, taken(0, span)), (-1, span, taken(1, span))), (rising, falling)
        )
        rising, falling = up(rising), down(falling)
        mine, other = joined(spots, partials, span, rising, falling)
        parts += [mine, swap(other)]

    sums, batches = (), []
    for names in (("0", "1u"), ("1d", "2u"), ("2d", "3u"), ("3d", "4u")):
        group = [near[name] for name in names]
        pieces = [piece for _, piece, _ in group] + [piece for _, _, piece in group]
        marks = tuple((shift, swapped) for swapped in (False, True) for shift, _, _ in group)
        normed, total = normalized(marks, spots, pieces, partials, gain_row, sums)
        sums = (total,)
        batches.append((marks, normed))
    out = ()
    for batch in (batches[:1], batches[1:2], batches[2:3], batches[3:]):
        marks, normed = zip(*batch)
        out = (
            project(marks, spots, normed, qkv_weight, bias_row, cosine, sine, out),
        )

    total = summed(total, swap(total))

    def across(reach):
        return lax.ppermute(total, "mp_0", [(i, i ^ reach) for i in range(RING)])

    total = summed(total, across(4))
    sums = (total, across(1), across(2), across(3))

    bias_grad, parts[2] = lax.optimization_barrier((bias_grad, parts[2]))
    tokens_grad, total = finished(tokens, gain_row, parts, sums)
    return (out[0], tokens_grad, total[0], bias_grad[0])


def solution(mesh):
    split = Mesh(mesh.devices.reshape(mesh.shape["dp"], 8, 2), ("dp", "mp_0", "mp_1"))
    placed = (P(DP_MP, None), P(), P(None, MP), P(MP), P("dp", MP))
    return jax.shard_map(
        work,
        mesh=split,
        in_specs=placed,
        out_specs=(P("dp", MP), P(DP_MP, None), P("dp"), P(DP_MP)),
        check_vma=False,
    )
```
